32 devices in a mesh: slab: 8 (over z, y), pencil: 4 (over x, core).
Axes of the slice: x: 2, y: 2, z: 4, core: 2. Of those that a mesh axis runs over, the one named last changes fastest.
Arguments:
- density_history: float32 [7, 64, 320, 320], P(None, 'slab', 'pencil'), may hold values from -6 to 6
- residual_history: float32 [7, 64, 320, 320], P(None, 'slab', 'pencil'), as said below
- occupancy_history: float32 [7, 768, 324], P(None, ('slab', 'pencil')), may hold values from -6 to 6
- occupancy_residual: float32 [7, 768, 324], P(None, ('slab', 'pencil')), may hold values from -6 to 6
- species: int32 [768], P(('slab', 'pencil')), may hold values from 0 to 3
- slot_count: int32 [32], P(('slab', 'pencil')), may hold values from 12 to 24, as said below
Outputs:
- new_density: float32 [64, 320, 320], P('slab', 'pencil')
- new_occupancy: float32 [768, 324], P(('slab', 'pencil'))
The draws below stay inside these ranges and needn't reach their ends.
Inputs may be any that keep to these rules, and one draw needn't show every extreme that they name: `residual_history`: residual fields of the 7 previous steps. Device d of slab+pencil (slab slowest) holds slots d * 24 to (d + 1) * 24 - 1, of which the first slot_count[d] hold atoms; some device is full in every draw.
All inputs are finite; a program needn't handle non-finite values.
Results may differ from the reference program's by a relative error of at most 0.00017.
Values sent between devices are 32-bit elements; how exact they have to be, the bound alone decides.
A program may use at most 128 MiB of HBM per device.

```python
import math
import jax
import jax.numpy as jnp
from jax import lax

HISTORY = 7
NX = 320
NY = 320
NZ = 64
ORBITALS = 18
SLOT_DEV = 24
SLOTS = 768


def smooth_lines(key, leading, length):
    keys = jax.random.split(key, 2)
    amplitude = 0.5 * jax.random.normal(keys[0], leading + (4,), jnp.float32)
    phase = jax.random.uniform(keys[1], leading + (4,), jnp.float32, 0.0, 2.0 * math.pi)
    position = jnp.arange(length, dtype=jnp.float32)
    wavenumber = jnp.arange(1, 5, dtype=jnp.float32)
    angle = 2.0 * math.pi * wavenumber[:, None] * position[None, :] / length
    return jnp.sum(amplitude[..., None] * jnp.cos(angle + phase[..., None]), axis=-2)


def region_scale(key, length, upper):
    return jnp.exp(jax.random.uniform(key, (length,), jnp.float32, 0.0, math.log(upper)))


def draw_residual_history(key, part):
    keys = jax.random.split(key, 11)
    shared = 0.6
    spread = 4.0
    upper = 3.0
    common_noise = jax.random.normal(keys[0], (NZ, NY, NX), jnp.float32)
    own_noise = jax.random.normal(keys[1], (HISTORY, NZ, NY, NX), jnp.float32)
    region = region_scale(keys[2], NZ, upper)[:, None, None] * region_scale(keys[3], NY, upper)[None, :, None] * region_scale(keys[4], NX, upper)[None, None, :]
    common_smooth = smooth_lines(keys[5], (), NZ)[:, None, None] + smooth_lines(keys[6], (), NY)[None, :, None] + smooth_lines(keys[7], (), NX)[None, None, :]
    own_smooth = smooth_lines(keys[8], (HISTORY,), NZ)[:, :, None, None] + smooth_lines(keys[9], (HISTORY,), NY)[:, None, :, None] + smooth_lines(keys[10], (HISTORY,), NX)[:, None, None, :]
    common = common_noise * region + common_smooth
    own = own_noise * region[None] + own_smooth
    step_index = jnp.arange(HISTORY, dtype=jnp.float32)
    history_scale = jnp.exp(math.log(spread) * (1.0 - step_index / max(HISTORY - 1, 1)))
    value = history_scale[:, None, None, None] * (shared * common[None] + math.sqrt(1.0 - shared * shared) * own)
    return value.astype(jnp.float32)


def draw_slot_count(key, part):
    keys = jax.random.split(key, 2)
    devices_total = SLOTS // SLOT_DEV
    counts = jax.random.randint(keys[0], (devices_total,), max(1, SLOT_DEV // 2), SLOT_DEV + 1)
    filled = jax.random.randint(keys[1], (), 0, devices_total)
    position = jnp.arange(devices_total, dtype=jnp.int32)
    return jnp.where(position == filled, SLOT_DEV, counts).astype(jnp.int32)


def set_ends(result, stream_key, least, top_value):
    spot = [jax.random.randint(jax.random.fold_in(stream_key, axis), (), 0, length) for axis, length in enumerate(result.shape)]
    main_axis = result.shape.index(max(result.shape))
    next_to = spot[:main_axis] + [(spot[main_axis] + 1) % result.shape[main_axis]] + spot[main_axis + 1:]
    return result.at[tuple(spot)].set(least).at[tuple(next_to)].set(top_value)


def block_levels(key, shape, cuts, least, largest):
    gain = 1.0
    for axis_at, parts in cuts:
        draws = jax.random.uniform(jax.random.fold_in(jax.random.fold_in(key, 6), axis_at), (parts,), jnp.float32, least / len(cuts), largest / len(cuts))
        gain = gain * jnp.repeat(jnp.exp(draws), shape[axis_at] // parts).reshape((-1,) + (1,) * (len(shape) - 1 - axis_at))
    return gain


def gaussian(key, shape, width, reach, cuts=(), kind=jnp.bfloat16):
    drawn = jax.random.normal(key, shape, jnp.float32) * width
    if len(cuts) > 0:
        drawn = block_levels(key, shape, cuts, -0.22, 0.18) * drawn
    return jnp.clip(drawn, min=-reach, max=reach).astype(kind)


def setup_inputs(seed: int = 0) -> dict:
    key_of = jax.random.split(jax.random.key(seed), 7)
    return {
        "density_history": gaussian(key_of[0], (HISTORY, NZ, NY, NX), 1.0, 6.0, ((1, 8), (2, 4)), jnp.float32),
        "residual_history": draw_residual_history(jax.random.fold_in(key_of[6], 71), 0),
        "occupancy_history": gaussian(key_of[2], (HISTORY, SLOTS, ORBITALS * ORBITALS), 1.0, 6.0, ((1, 32),), jnp.float32),
        "occupancy_residual": gaussian(key_of[3], (HISTORY, SLOTS, ORBITALS * ORBITALS), 1.0, 6.0, ((1, 32),), jnp.float32),
        "species": set_ends(jax.random.randint(key_of[4], (SLOTS,), 0, 4), jax.random.fold_in(key_of[4], 1), 0, 3).astype(jnp.int32),
        "slot_count": draw_slot_count(jax.random.fold_in(key_of[6], 71), 0),
    }


highest = lax.Precision.HIGHEST
grid_mixing = 0.5
block_mixing = 0.5
kerker_wave = 6.0
species_orbitals = (18, 13, 8, 5)

def block_mask(species, slot_count):
    position = jnp.arange(species.shape[0], dtype=jnp.int32)
    owner_count = slot_count[(position // SLOT_DEV).astype(jnp.int32)]
    live = position % SLOT_DEV < owner_count
    orbitals = jnp.zeros_like(species)
    for species_index, orbital_number in enumerate(species_orbitals):
        orbitals = orbitals + orbital_number * (species == species_index).astype(jnp.int32)
    entry = jnp.arange(ORBITALS * ORBITALS, dtype=jnp.int32)
    row_index = entry // ORBITALS
    column_index = entry % ORBITALS
    inside = (row_index[None, :] < orbitals[:, None]) & (column_index[None, :] < orbitals[:, None]) & live[:, None]
    return inside.astype(jnp.float32)

def mixing_weights(intersection):
    factor = jnp.linalg.cholesky(intersection)
    column = jnp.ones((intersection.shape[0], 1), intersection.dtype)
    middle = lax.linalg.triangular_solve(factor, column, left_side=True, lower=True)
    solved = lax.linalg.triangular_solve(factor, middle, left_side=True, lower=True, transpose_a=True)
    return solved[:, 0] / jnp.sum(solved)

def magnitude(length):
    index = jnp.arange(length, dtype=jnp.int32)
    return jnp.minimum(index, length - index).astype(jnp.float32)

def reference(density_history, residual_history, occupancy_history, occupancy_residual, species, slot_count):
    mask = block_mask(species, slot_count)
    flat = residual_history.reshape(HISTORY, -1)
    grid_intersection = jnp.dot(flat, flat.T, precision=highest) / (NX * NY * NZ)
    blocks = (occupancy_residual * mask[None]).reshape(HISTORY, -1)
    block_intersection = jnp.dot(blocks, blocks.T, precision=highest) / (100.0 * SLOTS)
    weights = mixing_weights(grid_intersection + block_intersection)
    mixed = jnp.tensordot(weights, residual_history, axes=1, precision=highest)
    spectrum = jnp.fft.fftn(mixed)
    square = magnitude(NZ)[:, None, None] ** 2 + magnitude(NY)[None, :, None] ** 2 + magnitude(NX)[None, None, :] ** 2
    factor = square / (square + kerker_wave * kerker_wave)
    filtered = jnp.real(jnp.fft.ifftn(spectrum * factor)).astype(jnp.float32)
    new_density = jnp.tensordot(weights, density_history, axes=1, precision=highest) + grid_mixing * filtered
    mixed_blocks = jnp.tensordot(weights, occupancy_history + block_mixing * occupancy_residual, axes=1, precision=highest)
    return (new_density, mask * mixed_blocks)
```

```python
import functools
import math

import jax
import jax.numpy as jnp
import numpy as np
from jax import lax
from jax.experimental import pallas as pl
from jax.experimental.pallas import tpu as pltpu
from jax.sharding import PartitionSpec as P

ORBITALS = 18


highest = lax.Precision.HIGHEST
grid_mixing = 0.5
block_mixing = 0.5
kerker_wave = 6.0
species_orbitals = (18, 13, 8, 5)


def block_mask(species, slot_count):
    live = jnp.arange(species.shape[0], dtype=jnp.int32) < slot_count[0]
    orbitals = jnp.zeros_like(species)
    for species_index, orbital_number in enumerate(species_orbitals):
        orbitals = orbitals + orbital_number * (species == species_index).astype(jnp.int32)
    entry = jnp.arange(ORBITALS * ORBITALS, dtype=jnp.int32)
    row_index = entry // ORBITALS
    column_index = entry % ORBITALS
    inside = (
        (row_index[None, :] < orbitals[:, None])
        & (column_index[None, :] < orbitals[:, None])
        & live[:, None]
    )
    return inside.astype(jnp.float32)


def mixing_weights(intersection):
    factor = jnp.linalg.cholesky(intersection)
    column = jnp.ones((intersection.shape[0], 1), intersection.dtype)
    middle = lax.linalg.triangular_solve(factor, column, left_side=True, lower=True)
    solved = lax.linalg.triangular_solve(
        factor, middle, left_side=True, lower=True, transpose_a=True
    )
    return solved[:, 0] / jnp.sum(solved)


def cosine_sine(length, freq_index, space_index):
    product = freq_index * space_index % length
    angle = 2.0 * math.pi / length * product.astype(jnp.float32)
    return (jnp.cos(angle), jnp.sin(angle))


def forward_spectra(fields, pencil_move, slab_move):
    batches, z_local, y_local, x_length = fields.shape
    pencil_count = lax.axis_size("pencil")
    slab_count = lax.axis_size("slab")
    x_columns = x_length // 2
    kx_local = x_columns // pencil_count
    y_length = y_local * pencil_count
    ky_local = y_length // slab_count
    z_length = z_local * slab_count
    freq_index = jnp.arange(x_columns, dtype=jnp.int32).reshape(pencil_count, kx_local, 1)
    space_index = jnp.arange(x_length, dtype=jnp.int32).reshape(1, 1, x_length)
    cosine, sine = cosine_sine(x_length, freq_index, space_index)
    nyquist = cosine_sine(x_length, jnp.full((1, 1, 1), x_length // 2, jnp.int32), space_index)[0]
    sine = jnp.where(freq_index == 0, -nyquist, sine)
    real_part = jnp.einsum("bzyx,pkx->bpkzy", fields, cosine, precision=highest)
    imag_part = -jnp.einsum("bzyx,pkx->bpkzy", fields, sine, precision=highest)
    packed = jnp.stack((real_part, imag_part), axis=1).reshape(batches, 2, pencil_count, -1)
    moved = pencil_move(packed).reshape(batches, 2, pencil_count, kx_local, z_local, y_local)
    freq_index = jnp.arange(y_length, dtype=jnp.int32).reshape(slab_count, ky_local, 1, 1)
    space_index = jnp.arange(y_length, dtype=jnp.int32).reshape(1, 1, pencil_count, y_local)
    cosine, sine = cosine_sine(y_length, freq_index, space_index)
    real_input = moved[:, 0]
    imag_input = moved[:, 1]
    form = "bskzy,glsy->bgklz"
    real_part = jnp.einsum(form, real_input, cosine, precision=highest) + jnp.einsum(
        form, imag_input, sine, precision=highest
    )
    imag_part = jnp.einsum(form, imag_input, cosine, precision=highest) - jnp.einsum(
        form, real_input, sine, precision=highest
    )
    packed = jnp.stack((real_part, imag_part), axis=1).reshape(batches, 2, slab_count, -1)
    moved = slab_move(packed).reshape(batches, 2, slab_count, kx_local, ky_local, z_local)
    freq_index = jnp.arange(z_length, dtype=jnp.int32).reshape(z_length, 1, 1)
    space_index = jnp.arange(z_length, dtype=jnp.int32).reshape(1, slab_count, z_local)
    cosine, sine = cosine_sine(z_length, freq_index, space_index)
    real_input = moved[:, 0]
    imag_input = moved[:, 1]
    form = "bgklz,mgz->bklm"
    real_part = jnp.einsum(form, real_input, cosine, precision=highest) + jnp.einsum(
        form, imag_input, sine, precision=highest
    )
    imag_part = jnp.einsum(form, imag_input, cosine, precision=highest) - jnp.einsum(
        form, real_input, sine, precision=highest
    )
    return jnp.stack((real_part, imag_part), axis=1)


def magnitude(index, length):
    return jnp.minimum(index, length - index).astype(jnp.float32)


def kerker_factor(freq_x, ky_local, x_length, y_length, z_length):
    freq_y = lax.axis_index("slab") * ky_local + jnp.arange(ky_local, dtype=jnp.int32)
    freq_z = jnp.arange(z_length, dtype=jnp.int32)
    square = (
        magnitude(freq_x, x_length)[:, None, None] ** 2
        + magnitude(freq_y, y_length)[None, :, None] ** 2
        + magnitude(freq_z, z_length)[None, None, :] ** 2
    )
    return square / (square + kerker_wave * kerker_wave)


def inverse_field(spectrum, z_local, y_local, x_length):
    pencil_count = lax.axis_size("pencil")
    slab_count = lax.axis_size("slab")
    x_columns = x_length // 2
    kx_local = x_columns // pencil_count
    slots = spectrum.shape[1]
    y_length = y_local * pencil_count
    ky_local = y_length // slab_count
    z_length = z_local * slab_count
    freq_index = jnp.arange(z_length, dtype=jnp.int32).reshape(z_length, 1, 1)
    space_index = jnp.arange(z_length, dtype=jnp.int32).reshape(1, slab_count, z_local)
    cosine, sine = cosine_sine(z_length, freq_index, space_index)
    real_input = spectrum[0]
    imag_input = spectrum[1]
    form = "klm,mdz->dklz"
    real_part = jnp.einsum(form, real_input, cosine, precision=highest) - jnp.einsum(
        form, imag_input, sine, precision=highest
    )
    imag_part = jnp.einsum(form, real_input, sine, precision=highest) + jnp.einsum(
        form, imag_input, cosine, precision=highest
    )
    packed = jnp.stack((real_part, imag_part), axis=0).reshape(2, slab_count, -1)
    moved = lax.all_to_all(packed, "slab", split_axis=1, concat_axis=1, tiled=True).reshape(
        2, slab_count, slots, ky_local, z_local
    )
    freq_index = jnp.arange(y_length, dtype=jnp.int32).reshape(slab_count, ky_local, 1, 1)
    space_index = jnp.arange(y_length, dtype=jnp.int32).reshape(1, 1, pencil_count, y_local)
    cosine, sine = cosine_sine(y_length, freq_index, space_index)
    real_input = moved[0]
    imag_input = moved[1]
    form = "gklz,glqy->qkzy"
    real_part = jnp.einsum(form, real_input, cosine, precision=highest) - jnp.einsum(
        form, imag_input, sine, precision=highest
    )
    imag_part = jnp.einsum(form, real_input, sine, precision=highest) + jnp.einsum(
        form, imag_input, cosine, precision=highest
    )
    packed = jnp.stack((real_part, imag_part), axis=0).reshape(2, pencil_count, -1)
    moved = lax.all_to_all(packed, "pencil", split_axis=1, concat_axis=1, tiled=True).reshape(
        2, pencil_count, slots, z_local, y_local
    )
    pencil_index = jnp.arange(pencil_count, dtype=jnp.int32).reshape(pencil_count, 1, 1)
    slot_index = jnp.arange(slots, dtype=jnp.int32).reshape(1, slots, 1)
    space_index = jnp.arange(x_length, dtype=jnp.int32).reshape(1, 1, x_length)
    freq_index = pencil_index * kx_local + slot_index
    cosine, sine = cosine_sine(x_length, freq_index, space_index)
    nyquist = cosine_sine(x_length, jnp.full((1, 1, 1), x_length // 2, jnp.int32), space_index)[0]
    ordinary = slot_index < kx_local
    doubling = jnp.where(freq_index == 0, 1.0, 2.0)
    real_table = jnp.where(ordinary, doubling * cosine, 0.0)
    imag_table = jnp.where(ordinary, -doubling * sine, jnp.where(pencil_index == 0, nyquist, 0.0))
    form = "pkzy,pkx->zyx"
    field = jnp.einsum(form, moved[0], real_table, precision=highest) + jnp.einsum(
        form, moved[1], imag_table, precision=highest
    )
    return field / (x_length * y_length * z_length)


def body(
    density_history, residual_history, occupancy_history, occupancy_residual, species, slot_count
):
    histories, z_local, y_local, x_length = residual_history.shape
    slab_count = lax.axis_size("slab")
    pencil_count = lax.axis_size("pencil")
    cell_total = z_local * slab_count * y_local * pencil_count * x_length
    slot_total = species.shape[0] * slab_count * pencil_count
    mask = block_mask(species, slot_count)
    flat = residual_history.reshape(histories, -1)
    grid_local = jnp.dot(flat, flat.T, precision=highest) / cell_total
    blocks = (occupancy_residual * mask[None]).reshape(histories, -1)
    block_local = jnp.dot(blocks, blocks.T, precision=highest) / (100.0 * slot_total)
    grid_intersection, block_intersection = lax.psum((grid_local, block_local), ("slab", "pencil"))
    weights = mixing_weights(grid_intersection + block_intersection)
    mixed = jnp.tensordot(weights, residual_history, axes=1, precision=highest)
    spectrum = forward_spectra(
        mixed[None],
        lambda packed: lax.all_to_all(packed, "pencil", split_axis=2, concat_axis=2, tiled=True),
        lambda packed: lax.all_to_all(packed, "slab", split_axis=2, concat_axis=2, tiled=True),
    )[0]
    x_columns = x_length // 2
    kx_local = x_columns // pencil_count
    y_length = y_local * pencil_count
    z_length = z_local * slab_count
    ky_local = y_length // slab_count
    freq_x = lax.axis_index("pencil") * kx_local + jnp.arange(kx_local, dtype=jnp.int32)
    factor = kerker_factor(freq_x, ky_local, x_length, y_length, z_length)
    filtered_spectrum = spectrum * factor[None]
    nyquist_x = jnp.full((1,), x_length // 2, jnp.int32)
    nyquist_factor = kerker_factor(nyquist_x, ky_local, x_length, y_length, z_length)
    owner = (lax.axis_index("pencil") == 0).astype(jnp.float32)
    extra = spectrum[:, 0:1] * nyquist_factor[None] * owner
    filtered_spectrum = jnp.concatenate((filtered_spectrum, extra), axis=1)
    filtered = inverse_field(filtered_spectrum, z_local, y_local, x_length)
    new_density = (
        jnp.tensordot(weights, density_history, axes=1, precision=highest) + grid_mixing * filtered
    )
    mixed_blocks = jnp.tensordot(
        weights, occupancy_history + block_mixing * occupancy_residual, axes=1, precision=highest
    )
    return (new_density, mask * mixed_blocks)


MESH = pl.DeviceIdType.MESH
VMEM_LIMIT = 40000 * 1024


def split(value):
    high = value.astype(jnp.bfloat16)
    low = (value - high.astype(jnp.float32)).astype(jnp.bfloat16)
    return high, low


def three(left, right, dims):
    numbers = (dims, ((), ()))
    dot = functools.partial(
        lax.dot_general, dimension_numbers=numbers, preferred_element_type=jnp.float32
    )
    return dot(left[1], right[0]) + dot(left[0], right[1]) + dot(left[0], right[0])


def halves(table):
    table = np.asarray(table, np.float32)
    high = table.astype(jnp.bfloat16)
    low = (table - high.astype(np.float32)).astype(jnp.bfloat16)
    return np.stack((high, low))


def waves(rows, columns, length):
    angle = 2.0 * np.pi / length * (np.outer(rows, columns) % length)
    return np.cos(angle), np.sin(angle)


def tables(x_length, y_length, z_length, pencil_count, slab_count):
    columns = x_length // 2
    cosine, sine = waves(np.arange(columns), np.arange(x_length), x_length)
    nyquist = np.where(np.arange(x_length) % 2 == 0, 1.0, -1.0)
    imag = -sine
    imag[0] = nyquist
    slots_k = columns // (pencil_count * slab_count)
    owner, slot = np.arange(columns) // slots_k, np.arange(columns) % slots_k
    chunk = np.searchsorted(cuts_of(slots_k), slot, side="right")
    order = np.lexsort((slot, owner, chunk))
    x_forward = np.stack((cosine, imag), axis=1)[order].reshape(x_length, x_length)
    doubling = np.where(np.arange(columns) == 0, 1.0, 2.0)[:, None]
    back = np.stack((doubling * cosine, doubling * imag), axis=1)[order]
    back = back.reshape(x_length, x_length)
    x_back = back * (grid_mixing / (x_length * y_length * z_length))
    cosine, sine = waves(np.arange(y_length), np.arange(y_length), y_length)
    along_y = np.stack((cosine, sine))
    cosine, sine = waves(np.arange(z_length), np.arange(z_length), z_length)
    order = np.arange(z_length).reshape(slab_count, -1).T.reshape(-1)
    cosine, sine = cosine[:, order], sine[:, order]
    z_forward = np.block([[cosine, sine], [-sine, cosine]])
    z_back = np.block([[cosine.T, -sine.T], [sine.T, cosine.T]])
    return [halves(t) for t in (x_forward, x_back, along_y, z_forward, z_back)]


def cuts_of(slots):
    return [at for at in range(1, slots, 2)] + [slots]


def pairs_of(count):
    return [(i, j) for i in range(count) for j in range(i + 1)]


def solve_weights(entry, count):
    lower, pivot = {}, []
    for j in range(count):
        scaled = [lower[j, k] * pivot[k] for k in range(j)]
        value = entry[j, j]
        for k in range(j):
            value = value - lower[j, k] * scaled[k]
        pivot.append(value)
        for i in range(j + 1, count):
            value = entry[i, j]
            for k in range(j):
                value = value - lower[i, k] * scaled[k]
            lower[i, j] = value / pivot[j]
    middle = []
    for i in range(count):
        value = jnp.ones_like(pivot[0])
        for k in range(i):
            value = value - lower[i, k] * middle[k]
        middle.append(value)
    solved = [None] * count
    for i in reversed(range(count)):
        value = middle[i] / pivot[i]
        for k in range(i + 1, count):
            value = value - lower[k, i] * solved[k]
        solved[i] = value
    total = solved[0]
    for value in solved[1:]:
        total = total + value
    return [value / total for value in solved]


def mix_kernel(
    slabs, pencils, cells, slots,
    live_ref, res_hbm, dens_hbm, occ_hbm, occ_res_hbm, species_hbm, corner_hbm,
    xf_hbm, yt_hbm, zf_hbm, zb_hbm, xb_hbm,
    out_ref, occ_out_ref,
    res, dens, occ_ref, occ_res_ref, species_ref, corner_ref,
    first_turn, sums, send_box, land_box, planes, spectrum, back_box, field,
    xf_ref, yt_ref, zf_ref, zb_ref, xb_ref,
    res_sem, table_sem, sum_sem, go_send, go_recv, back_send, back_recv,
):
    devices = slabs * pencils
    count, z_local, y_local, x_length = res.shape
    slots_k = x_length // 2 // devices
    freqs = 2 * slots_k
    z_length = z_local * slabs
    y_length = y_local * pencils
    tiles_out = send_box.shape[0]
    slab = lax.axis_index("slab")
    pencil = lax.axis_index("pencil")
    me = slab * pencils + pencil
    pairs = pairs_of(count)
    ends = cuts_of(slots_k)
    chunks = list(zip([0] + ends[:-1], ends))

    def place(index):
        return (lax.div(index, pencils), lax.rem(index, pencils))

    def other(step):
        return lax.rem(me + step, devices)

    sources = (
        occ_res_hbm, species_hbm, corner_hbm, xf_hbm,
        occ_hbm, dens_hbm, yt_hbm, zf_hbm, zb_hbm, xb_hbm,
    )
    targets = (
        occ_res_ref, species_ref, corner_ref, xf_ref,
        occ_ref, dens, yt_ref, zf_ref, zb_ref, xb_ref,
    )
    loads = [
        pltpu.make_async_copy(a, b, table_sem.at[at])
        for at, (a, b) in enumerate(zip(sources, targets))
    ]
    res_loads = [
        pltpu.make_async_copy(res_hbm.at[:, z], res.at[:, z], res_sem.at[z])
        for z in range(z_local)
    ]
    for copy in loads[:3] + res_loads + loads[3:4]:
        copy.start()

    barrier = pltpu.get_barrier_semaphore()

    def greet(step, _):
        pl.semaphore_signal(
            barrier, inc=1, device_id=place(other(step)), device_id_type=MESH
        )
        return 0

    lax.fori_loop(1, devices, greet, 0)

    def wide(value):
        width = value.shape[1]
        if width == 128:
            return value
        return jnp.concatenate((value, jnp.zeros((8, 128 - width), value.dtype)), axis=1)

    def lanes_of(length):
        return [(at, min(at + 128, length)) for at in range(0, length, 128)]

    for copy in loads[:3]:
        copy.wait()
    slot_count, entries = occ_ref.shape[1:]
    species = species_ref[...]
    orbitals = jnp.zeros_like(species)
    for species_index, orbital_number in enumerate(species_orbitals):
        orbitals = jnp.where(species == species_index, orbital_number, orbitals)
    square = (slot_count, slot_count)
    row_index = lax.broadcasted_iota(jnp.int32, square, 0)
    column_index = lax.broadcasted_iota(jnp.int32, square, 1)
    chosen = (row_index == column_index) & (column_index < live_ref[0])
    limit = jnp.sum(
        jnp.where(chosen, orbitals.astype(jnp.float32), 0.0), axis=1, keepdims=True
    )
    mask = (corner_ref[...] < limit).astype(jnp.float32)
    ratio = cells / (100.0 * slots)
    acc = [jnp.zeros((8, 128), jnp.float32) for _ in pairs]
    for first in range(0, slot_count, 8):
        for start, stop in lanes_of(entries):
            part = [
                wide(occ_res_ref[i, first:first + 8, start:stop] * mask[first:first + 8, start:stop])
                for i in range(count)
            ]
            for at, (i, j) in enumerate(pairs):
                acc[at] = acc[at] + part[i] * part[j]
    acc = [value * ratio for value in acc]
    for z in range(z_local):
        res_loads[z].wait()

        def rows(step, acc):
            acc = list(acc)
            row = pl.multiple_of(step * 8, 8)
            for start, stop in lanes_of(x_length):
                part = [wide(res[i, z, pl.ds(row, 8), start:stop]) for i in range(count)]
                for at, (i, j) in enumerate(pairs):
                    acc[at] = acc[at] + part[i] * part[j]
            return tuple(acc)

        acc = lax.fori_loop(0, y_local // 8, rows, tuple(acc))
    for copy in loads[4:]:
        copy.start()
    stacked = jnp.concatenate([jnp.sum(a, axis=0, keepdims=True) for a in acc], axis=0)
    totals = jnp.sum(stacked, axis=1, keepdims=True) / cells
    shape = (len(pairs), 128)
    pair_index = lax.broadcasted_iota(jnp.int32, shape, 0)
    across = lax.broadcasted_iota(jnp.int32, shape, 1)
    packed = jnp.sum(jnp.where(pair_index == across, totals, 0.0), axis=0, keepdims=True)
    sums[pl.ds(me, 1), :] = packed

    pl.semaphore_wait(barrier, devices - 1)

    def sum_copy(source, target):
        return pltpu.make_async_remote_copy(
            src_ref=sums.at[pl.ds(source, 1)], dst_ref=sums.at[pl.ds(source, 1)],
            send_sem=sum_sem.at[0], recv_sem=sum_sem.at[1],
            device_id=place(target), device_id_type=MESH,
        )

    def start_sum(step, _):
        sum_copy(me, other(step)).start()
        return 0

    lax.fori_loop(1, devices, start_sum, 0)
    all_sums = pltpu.make_async_remote_copy(
        src_ref=sums.at[pl.ds(0, devices - 1)], dst_ref=sums.at[pl.ds(0, devices - 1)],
        send_sem=sum_sem.at[0], recv_sem=sum_sem.at[1],
        device_id=place(other(1)), device_id_type=MESH,
    )

    loads[3].wait()
    opening = slice(0, 2 * ends[0] * devices)

    def turn(i, _):
        history = split(res[i].reshape(z_local * y_local, x_length))
        left = (xf_ref[0, opening, :], xf_ref[1, opening, :])
        first_turn[i] = three(left, history, ((1,), (1,)))
        return 0

    lax.fori_loop(0, count, turn, 0)

    all_sums.wait_recv()
    gathered = jnp.sum(sums[...], axis=0, keepdims=True)
    lane_index = lax.broadcasted_iota(jnp.int32, (1, 128), 1)
    entry = {
        pair: jnp.sum(jnp.where(lane_index == at, gathered, 0.0), axis=1, keepdims=True)
        for at, pair in enumerate(pairs)
    }
    weights = solve_weights(entry, count)

    def share(chunk, index):
        first, end = chunks[chunk]
        size = 2 * (end - first)
        return pl.ds(2 * first * devices + index * size, size)

    def go_copy(chunk, source, target):
        return pltpu.make_async_remote_copy(
            src_ref=send_box.at[:, share(chunk, target), :],
            dst_ref=land_box.at[:, share(chunk, source), :],
            send_sem=go_send.at[0], recv_sem=go_recv.at[chunk],
            device_id=place(target), device_id_type=MESH,
        )

    def back_copy(chunk, source, target):
        return pltpu.make_async_remote_copy(
            src_ref=back_box.at[:, share(chunk, target), :],
            dst_ref=field.at[:, share(chunk, source), :],
            send_sem=back_send.at[0], recv_sem=back_recv.at[chunk],
            device_id=place(target), device_id_type=MESH,
        )

    def start_all(copy, chunk):
        def start(step, _):
            copy(chunk, me, other(step)).start()
            return 0

        lax.fori_loop(1, devices, start, 0)

    def whole(source, target, rows, send, recv):
        return pltpu.make_async_remote_copy(
            src_ref=source.at[:, rows, :], dst_ref=target.at[:, rows, :],
            send_sem=send, recv_sem=recv, device_id=place(other(1)), device_id_type=MESH,
        )

    def land_all(source, target, send, recv, chunk):
        first, end = chunks[chunk]
        rows = pl.ds(2 * first * devices, 2 * (end - first) * (devices - 1))
        whole(source, target, rows, send.at[0], recv.at[chunk]).wait_recv()

    def drain_all(source, target, send, recv):
        rows = pl.ds(0, freqs * (devices - 1))
        whole(source, target, rows, send.at[0], recv.at[0]).wait_send()

    def mixed(parts):
        total = weights[0] * parts[0]
        for i in range(1, count):
            total = total + weights[i] * parts[i]
        return total

    turned = mixed([first_turn[i] for i in range(count)])
    for t in range(tiles_out):
        send_box[t, opening, :] = turned[:, t * 128:(t + 1) * 128]
    start_all(go_copy, 0)
    land_box[:, share(0, me), :] = send_box[:, share(0, me), :]

    mixture = [mixed([res[i, z] for i in range(count)]) for z in range(z_local)]
    mixture = split(jnp.concatenate(mixture, axis=0))
    for chunk, (first, end) in enumerate(chunks):
        if chunk == 0:
            continue
        rows = slice(2 * first * devices, 2 * end * devices)
        turned = three((xf_ref[0, rows, :], xf_ref[1, rows, :]), mixture, ((1,), (1,)))
        for t in range(tiles_out):
            send_box[t, rows, :] = turned[:, t * 128:(t + 1) * 128]
        start_all(go_copy, chunk)
        land_box[:, share(chunk, me), :] = send_box[:, share(chunk, me), :]

    for copy in loads[4:]:
        copy.wait()
    for z in range(z_local):
        out_ref[z * y_local:(z + 1) * y_local, :] = mixed([dens[i, z] for i in range(count)])
    occ_out_ref[...] = mask * mixed(
        [occ_ref[i] + block_mixing * occ_res_ref[i] for i in range(count)]
    )
    all_sums.wait_send()

    z_forward = (zf_ref[0], zf_ref[1])
    z_back = (zb_ref[0], zb_ref[1])
    y_cosine = (yt_ref[0, 0], yt_ref[1, 0])
    y_sine = (yt_ref[0, 1], yt_ref[1, 1])
    shape = (2 * z_length, y_length)
    z_index = lax.rem(lax.broadcasted_iota(jnp.int32, shape, 0), z_length)
    y_index = lax.broadcasted_iota(jnp.int32, shape, 1)
    z_size = jnp.minimum(z_index, z_length - z_index).astype(jnp.float32)
    y_size = jnp.minimum(y_index, y_length - y_index).astype(jnp.float32)
    flat = z_size * z_size + y_size * y_size

    def filtered(wave, freq_x):
        size = freq_x.astype(jnp.float32)
        square = flat + size * size
        return split(wave * (square / (square + kerker_wave * kerker_wave)))

    for chunk, (first, end) in enumerate(chunks):
        size = 2 * (end - first)
        base = 2 * first * devices
        land_all(send_box, land_box, go_send, go_recv, chunk)
        for p in range(pencils):
            for f in range(size):
                joined = jnp.concatenate(
                    [
                        land_box[t, pl.ds(base + p * size + f, slabs, stride=pencils * size), :]
                        for t in range(tiles_out)
                    ],
                    axis=1,
                )
                for z in range(z_local):
                    planes[
                        2 * first + f, z * slabs:(z + 1) * slabs, p * y_local:(p + 1) * y_local
                    ] = joined[:, z * y_local:(z + 1) * y_local]
        block = split(planes[2 * first:2 * end].reshape(size * z_length, y_length))
        along_cosine = three(block, y_cosine, ((1,), (0,)))
        along_sine = three(block, y_sine, ((1,), (0,)))
        extra = first == 0
        for k in range(first, end):
            top, low = 2 * (k - first) * z_length, (2 * (k - first) + 1) * z_length
            stop = low + z_length
            real = along_cosine[top:low] + along_sine[low:stop]
            imag = along_cosine[low:stop] - along_sine[top:low]
            wave = three(z_forward, split(jnp.concatenate((real, imag), axis=0)), ((1,), (0,)))
            freq_x = me * slots_k + k
            spectrum[k - first] = three(z_back, filtered(wave, freq_x), ((1,), (0,)))
            if k == 0:
                freq_x = jnp.where(me == 0, x_length // 2, freq_x)
                spectrum[end] = three(z_back, filtered(wave, freq_x), ((1,), (0,)))
        used = end - first + (1 if extra else 0)
        block = split(spectrum[0:used].reshape(used * 2 * z_length, y_length))
        along_cosine = three(block, y_cosine, ((1,), (0,)))
        along_sine = three(block, y_sine, ((1,), (0,)))
        for k in range(first, end):
            top, low = 2 * (k - first) * z_length, (2 * (k - first) + 1) * z_length
            stop = low + z_length
            real = along_cosine[top:low] - along_sine[low:stop]
            if k == 0:
                top, low = 2 * end * z_length, (2 * end + 1) * z_length
                stop = low + z_length
            imag = along_cosine[low:stop] + along_sine[top:low]
            for c, part in enumerate((real, imag)):
                for p in range(pencils):
                    joined = jnp.concatenate(
                        [
                            part[z * slabs:(z + 1) * slabs, p * y_local:(p + 1) * y_local]
                            for z in range(z_local)
                        ],
                        axis=1,
                    )
                    start = base + p * size + 2 * (k - first) + c
                    for t in range(tiles_out):
                        back_box[t, pl.ds(start, slabs, stride=pencils * size), :] = joined[
                            :, t * 128:(t + 1) * 128
                        ]
        start_all(back_copy, chunk)
        field[:, share(chunk, me), :] = back_box[:, share(chunk, me), :]

    drain_all(send_box, land_box, go_send, go_recv)
    for chunk, (first, end) in enumerate(chunks):
        land_all(back_box, field, back_send, back_recv, chunk)
        used = slice(2 * first * devices, 2 * end * devices)
        table = (xb_ref[0, used, :], xb_ref[1, used, :])
        for t in range(tiles_out):
            rows = slice(t * 128, (t + 1) * 128)
            out_ref[rows, :] = out_ref[rows, :] + three(
                split(field[t, used, :]), table, ((0,), (0,))
            )
    drain_all(back_box, field, back_send, back_recv)


def fused_body(
    density_history, residual_history, occupancy_history, occupancy_residual, species, slot_count
):
    count, z_local, y_local, x_length = residual_history.shape
    slabs = lax.axis_size("slab")
    pencils = lax.axis_size("pencil")
    devices = slabs * pencils
    z_length, y_length = z_local * slabs, y_local * pencils
    freqs = x_length // devices
    entry = np.arange(ORBITALS * ORBITALS)
    corner = np.maximum(entry // ORBITALS, entry % ORBITALS)[None].astype(np.float32)
    x_forward, x_back, *others = [
        jnp.asarray(t) for t in tables(x_length, y_length, z_length, pencils, slabs)
    ]
    constants = [x_forward, *others, x_back]
    ends = cuts_of(freqs // 2)
    chunks = len(ends)
    vmem = pl.BlockSpec(memory_space=pltpu.VMEM)
    hbm = pl.BlockSpec(memory_space=pltpu.HBM)
    box = (z_local * y_local // 128, devices * freqs, 128)
    sems = pltpu.SemaphoreType.DMA
    flat = jax.ShapeDtypeStruct((z_local * y_local, x_length), jnp.float32)
    blocks = jax.ShapeDtypeStruct(occupancy_history.shape[1:], jnp.float32)
    smalls = [
        occupancy_history, occupancy_residual, species[None], jnp.asarray(corner)
    ]
    new_density, new_blocks = pl.pallas_call(
        functools.partial(
            mix_kernel, slabs, pencils,
            z_length * y_length * x_length, species.shape[0] * devices,
        ),
        out_shape=(flat, blocks),
        in_specs=[pl.BlockSpec(memory_space=pltpu.SMEM)] + [hbm] * (6 + len(constants)),
        out_specs=(vmem, vmem),
        scratch_shapes=[
            pltpu.VMEM(residual_history.shape, jnp.float32),
            pltpu.VMEM(residual_history.shape, jnp.float32),
            *[pltpu.VMEM(t.shape, t.dtype) for t in smalls],
            pltpu.VMEM((count, 2 * ends[0] * devices, z_local * y_local), jnp.float32),
            pltpu.VMEM((devices, 128), jnp.float32),
            pltpu.VMEM(box, jnp.float32),
            pltpu.VMEM(box, jnp.float32),
            pltpu.VMEM((freqs, z_length, y_length), jnp.float32),
            pltpu.VMEM((freqs // 2 + 1, 2 * z_length, y_length), jnp.float32),
            pltpu.VMEM(box, jnp.float32),
            pltpu.VMEM(box, jnp.float32),
            *[pltpu.VMEM(t.shape, t.dtype) for t in constants],
            sems((z_local,)),
            sems((5 + len(constants),)),
            sems((2,)),
            sems((1,)), sems((chunks,)),
            sems((1,)), sems((chunks,)),
        ],
        compiler_params=pltpu.CompilerParams(
            collective_id=0, has_side_effects=True, vmem_limit_bytes=VMEM_LIMIT
        ),
    )(slot_count, *[
        pltpu.with_memory_space_constraint(value, pltpu.HBM)
        for value in (residual_history, density_history, *smalls, *constants)
    ])
    return new_density.reshape(z_local, y_local, x_length), new_blocks


def solution(mesh):
    placed = (
        P(None, "slab", "pencil", None),
        P(None, "slab", "pencil", None),
        P(None, ("slab", "pencil"), None),
        P(None, ("slab", "pencil"), None),
        P(("slab", "pencil")),
        P(("slab", "pencil")),
    )
    devices = mesh.shape["slab"] * mesh.shape["pencil"]

    def chosen(*arrays):
        x_length = arrays[0].shape[3]
        _, z_local, y_local, _ = arrays[0].shape
        fits = (
            x_length % (2 * devices) == 0
            and mesh.shape["slab"] % 8 == 0
            and y_local % 16 == 0
            and z_local * y_local % 128 == 0
        )
        return (fused_body if fits else body)(*arrays)

    return jax.shard_map(
        chosen,
        mesh=mesh,
        in_specs=placed,
        out_specs=(P("slab", "pencil", None), P(("slab", "pencil"), None)),
        check_vma=False,
    )
```

```python
import functools
import math

import jax
import jax.numpy as jnp
import numpy as np
from jax import lax
from jax.experimental import pallas as pl
from jax.experimental.pallas import tpu as pltpu
from jax.sharding import PartitionSpec as P

ORBITALS = 18


highest = lax.Precision.HIGHEST
grid_mixing = 0.5
block_mixing = 0.5
kerker_wave = 6.0
species_orbitals = (18, 13, 8, 5)


def block_mask(species, slot_count):
    live = jnp.arange(species.shape[0], dtype=jnp.int32) < slot_count[0]
    orbitals = jnp.zeros_like(species)
    for species_index, orbital_number in enumerate(species_orbitals):
        orbitals = orbitals + orbital_number * (species == species_index).astype(jnp.int32)
    entry = jnp.arange(ORBITALS * ORBITALS, dtype=jnp.int32)
    row_index = entry // ORBITALS
    column_index = entry % ORBITALS
    inside = (
        (row_index[None, :] < orbitals[:, None])
        & (column_index[None, :] < orbitals[:, None])
        & live[:, None]
    )
    return inside.astype(jnp.float32)


def mixing_weights(intersection):
    factor = jnp.linalg.cholesky(intersection)
    column = jnp.ones((intersection.shape[0], 1), intersection.dtype)
    middle = lax.linalg.triangular_solve(factor, column, left_side=True, lower=True)
    solved = lax.linalg.triangular_solve(
        factor, middle, left_side=True, lower=True, transpose_a=True
    )
    return solved[:, 0] / jnp.sum(solved)


def cosine_sine(length, freq_index, space_index):
    product = freq_index * space_index % length
    angle = 2.0 * math.pi / length * product.astype(jnp.float32)
    return (jnp.cos(angle), jnp.sin(angle))


def forward_spectra(fields, pencil_move, slab_move):
    batches, z_local, y_local, x_length = fields.shape
    pencil_count = lax.axis_size("pencil")
    slab_count = lax.axis_size("slab")
    x_columns = x_length // 2
    kx_local = x_columns // pencil_count
    y_length = y_local * pencil_count
    ky_local = y_length // slab_count
    z_length = z_local * slab_count
    freq_index = jnp.arange(x_columns, dtype=jnp.int32).reshape(pencil_count, kx_local, 1)
    space_index = jnp.arange(x_length, dtype=jnp.int32).reshape(1, 1, x_length)
    cosine, sine = cosine_sine(x_length, freq_index, space_index)
    nyquist = cosine_sine(x_length, jnp.full((1, 1, 1), x_length // 2, jnp.int32), space_index)[0]
    sine = jnp.where(freq_index == 0, -nyquist, sine)
    real_part = jnp.einsum("bzyx,pkx->bpkzy", fields, cosine, precision=highest)
    imag_part = -jnp.einsum("bzyx,pkx->bpkzy", fields, sine, precision=highest)
    packed = jnp.stack((real_part, imag_part), axis=1).reshape(batches, 2, pencil_count, -1)
    moved = pencil_move(packed).reshape(batches, 2, pencil_count, kx_local, z_local, y_local)
    freq_index = jnp.arange(y_length, dtype=jnp.int32).reshape(slab_count, ky_local, 1, 1)
    space_index = jnp.arange(y_length, dtype=jnp.int32).reshape(1, 1, pencil_count, y_local)
    cosine, sine = cosine_sine(y_length, freq_index, space_index)
    real_input = moved[:, 0]
    imag_input = moved[:, 1]
    form = "bskzy,glsy->bgklz"
    real_part = jnp.einsum(form, real_input, cosine, precision=highest) + jnp.einsum(
        form, imag_input, sine, precision=highest
    )
    imag_part = jnp.einsum(form, imag_input, cosine, precision=highest) - jnp.einsum(
        form, real_input, sine, precision=highest
    )
    packed = jnp.stack((real_part, imag_part), axis=1).reshape(batches, 2, slab_count, -1)
    moved = slab_move(packed).reshape(batches, 2, slab_count, kx_local, ky_local, z_local)
    freq_index = jnp.arange(z_length, dtype=jnp.int32).reshape(z_length, 1, 1)
    space_index = jnp.arange(z_length, dtype=jnp.int32).reshape(1, slab_count, z_local)
    cosine, sine = cosine_sine(z_length, freq_index, space_index)
    real_input = moved[:, 0]
    imag_input = moved[:, 1]
    form = "bgklz,mgz->bklm"
    real_part = jnp.einsum(form, real_input, cosine, precision=highest) + jnp.einsum(
        form, imag_input, sine, precision=highest
    )
    imag_part = jnp.einsum(form, imag_input, cosine, precision=highest) - jnp.einsum(
        form, real_input, sine, precision=highest
    )
    return jnp.stack((real_part, imag_part), axis=1)


def magnitude(index, length):
    return jnp.minimum(index, length - index).astype(jnp.float32)


def kerker_factor(freq_x, ky_local, x_length, y_length, z_length):
    freq_y = lax.axis_index("slab") * ky_local + jnp.arange(ky_local, dtype=jnp.int32)
    freq_z = jnp.arange(z_length, dtype=jnp.int32)
    square = (
        magnitude(freq_x, x_length)[:, None, None] ** 2
        + magnitude(freq_y, y_length)[None, :, None] ** 2
        + magnitude(freq_z, z_length)[None, None, :] ** 2
    )
    return square / (square + kerker_wave * kerker_wave)


def inverse_field(spectrum, z_local, y_local, x_length):
    pencil_count = lax.axis_size("pencil")
    slab_count = lax.axis_size("slab")
    x_columns = x_length // 2
    kx_local = x_columns // pencil_count
    slots = spectrum.shape[1]
    y_length = y_local * pencil_count
    ky_local = y_length // slab_count
    z_length = z_local * slab_count
    freq_index = jnp.arange(z_length, dtype=jnp.int32).reshape(z_length, 1, 1)
    space_index = jnp.arange(z_length, dtype=jnp.int32).reshape(1, slab_count, z_local)
    cosine, sine = cosine_sine(z_length, freq_index, space_index)
    real_input = spectrum[0]
    imag_input = spectrum[1]
    form = "klm,mdz->dklz"
    real_part = jnp.einsum(form, real_input, cosine, precision=highest) - jnp.einsum(
        form, imag_input, sine, precision=highest
    )
    imag_part = jnp.einsum(form, real_input, sine, precision=highest) + jnp.einsum(
        form, imag_input, cosine, precision=highest
    )
    packed = jnp.stack((real_part, imag_part), axis=0).reshape(2, slab_count, -1)
    moved = lax.all_to_all(packed, "slab", split_axis=1, concat_axis=1, tiled=True).reshape(
        2, slab_count, slots, ky_local, z_local
    )
    freq_index = jnp.arange(y_length, dtype=jnp.int32).reshape(slab_count, ky_local, 1, 1)
    space_index = jnp.arange(y_length, dtype=jnp.int32).reshape(1, 1, pencil_count, y_local)
    cosine, sine = cosine_sine(y_length, freq_index, space_index)
    real_input = moved[0]
    imag_input = moved[1]
    form = "gklz,glqy->qkzy"
    real_part = jnp.einsum(form, real_input, cosine, precision=highest) - jnp.einsum(
        form, imag_input, sine, precision=highest
    )
    imag_part = jnp.einsum(form, real_input, sine, precision=highest) + jnp.einsum(
        form, imag_input, cosine, precision=highest
    )
    packed = jnp.stack((real_part, imag_part), axis=0).reshape(2, pencil_count, -1)
    moved = lax.all_to_all(packed, "pencil", split_axis=1, concat_axis=1, tiled=True).reshape(
        2, pencil_count, slots, z_local, y_local
    )
    pencil_index = jnp.arange(pencil_count, dtype=jnp.int32).reshape(pencil_count, 1, 1)
    slot_index = jnp.arange(slots, dtype=jnp.int32).reshape(1, slots, 1)
    space_index = jnp.arange(x_length, dtype=jnp.int32).reshape(1, 1, x_length)
    freq_index = pencil_index * kx_local + slot_index
    cosine, sine = cosine_sine(x_length, freq_index, space_index)
    nyquist = cosine_sine(x_length, jnp.full((1, 1, 1), x_length // 2, jnp.int32), space_index)[0]
    ordinary = slot_index < kx_local
    doubling = jnp.where(freq_index == 0, 1.0, 2.0)
    real_table = jnp.where(ordinary, doubling * cosine, 0.0)
    imag_table = jnp.where(ordinary, -doubling * sine, jnp.where(pencil_index == 0, nyquist, 0.0))
    form = "pkzy,pkx->zyx"
    field = jnp.einsum(form, moved[0], real_table, precision=highest) + jnp.einsum(
        form, moved[1], imag_table, precision=highest
    )
    return field / (x_length * y_length * z_length)


def body(
    density_history, residual_history, occupancy_history, occupancy_residual, species, slot_count
):
    histories, z_local, y_local, x_length = residual_history.shape
    slab_count = lax.axis_size("slab")
    pencil_count = lax.axis_size("pencil")
    cell_total = z_local * slab_count * y_local * pencil_count * x_length
    slot_total = species.shape[0] * slab_count * pencil_count
    mask = block_mask(species, slot_count)
    flat = residual_history.reshape(histories, -1)
    grid_local = jnp.dot(flat, flat.T, precision=highest) / cell_total
    blocks = (occupancy_residual * mask[None]).reshape(histories, -1)
    block_local = jnp.dot(blocks, blocks.T, precision=highest) / (100.0 * slot_total)
    grid_intersection, block_intersection = lax.psum((grid_local, block_local), ("slab", "pencil"))
    weights = mixing_weights(grid_intersection + block_intersection)
    mixed = jnp.tensordot(weights, residual_history, axes=1, precision=highest)
    spectrum = forward_spectra(
        mixed[None],
        lambda packed: lax.all_to_all(packed, "pencil", split_axis=2, concat_axis=2, tiled=True),
        lambda packed: lax.all_to_all(packed, "slab", split_axis=2, concat_axis=2, tiled=True),
    )[0]
    x_columns = x_length // 2
    kx_local = x_columns // pencil_count
    y_length = y_local * pencil_count
    z_length = z_local * slab_count
    ky_local = y_length // slab_count
    freq_x = lax.axis_index("pencil") * kx_local + jnp.arange(kx_local, dtype=jnp.int32)
    factor = kerker_factor(freq_x, ky_local, x_length, y_length, z_length)
    filtered_spectrum = spectrum * factor[None]
    nyquist_x = jnp.full((1,), x_length // 2, jnp.int32)
    nyquist_factor = kerker_factor(nyquist_x, ky_local, x_length, y_length, z_length)
    owner = (lax.axis_index("pencil") == 0).astype(jnp.float32)
    extra = spectrum[:, 0:1] * nyquist_factor[None] * owner
    filtered_spectrum = jnp.concatenate((filtered_spectrum, extra), axis=1)
    filtered = inverse_field(filtered_spectrum, z_local, y_local, x_length)
    new_density = (
        jnp.tensordot(weights, density_history, axes=1, precision=highest) + grid_mixing * filtered
    )
    mixed_blocks = jnp.tensordot(
        weights, occupancy_history + block_mixing * occupancy_residual, axes=1, precision=highest
    )
    return (new_density, mask * mixed_blocks)


MESH = pl.DeviceIdType.MESH
VMEM_LIMIT = 40000 * 1024


def split(value):
    high = value.astype(jnp.bfloat16)
    low = (value - high.astype(jnp.float32)).astype(jnp.bfloat16)
    return high, low


def three(left, right, dims):
    numbers = (dims, ((), ()))
    dot = functools.partial(
        lax.dot_general, dimension_numbers=numbers, preferred_element_type=jnp.float32
    )
    return dot(left[1], right[0]) + dot(left[0], right[1]) + dot(left[0], right[0])


def halves(table):
    table = np.asarray(table, np.float32)
    high = table.astype(jnp.bfloat16)
    low = (table - high.astype(np.float32)).astype(jnp.bfloat16)
    return np.stack((high, low))


def waves(rows, columns, length):
    angle = 2.0 * np.pi / length * (np.outer(rows, columns) % length)
    return np.cos(angle), np.sin(angle)


def tables(x_length, y_length, z_length, pencil_count, slab_count):
    columns = x_length // 2
    cosine, sine = waves(np.arange(columns), np.arange(x_length), x_length)
    nyquist = np.where(np.arange(x_length) % 2 == 0, 1.0, -1.0)
    imag = -sine
    imag[0] = nyquist
    slots_k = columns // (pencil_count * slab_count)
    owner, slot = np.arange(columns) // slots_k, np.arange(columns) % slots_k
    chunk = np.searchsorted(cuts_of(slots_k), slot, side="right")
    order = np.lexsort((slot, owner, chunk))
    x_forward = np.stack((cosine, imag), axis=1)[order].reshape(x_length, x_length)
    doubling = np.where(np.arange(columns) == 0, 1.0, 2.0)[:, None]
    back = np.stack((doubling * cosine, doubling * imag), axis=1)[order]
    back = back.reshape(x_length, x_length)
    x_back = back * (grid_mixing / (x_length * y_length * z_length))
    cosine, sine = waves(np.arange(y_length), np.arange(y_length), y_length)
    along_y = np.stack((cosine, sine))
    cosine, sine = waves(np.arange(z_length), np.arange(z_length), z_length)
    order = np.arange(z_length).reshape(slab_count, -1).T.reshape(-1)
    cosine, sine = cosine[:, order], sine[:, order]
    z_forward = np.block([[cosine, sine], [-sine, cosine]])
    z_back = np.block([[cosine.T, -sine.T], [sine.T, cosine.T]])
    return [halves(t) for t in (x_forward, x_back, along_y, z_forward, z_back)]


def cuts_of(slots):
    return [at for at in range(1, slots, 2)] + [slots]


def pairs_of(count):
    return [(i, j) for i in range(count) for j in range(i + 1)]


def solve_weights(entry, count):
    lower, pivot = {}, []
    for j in range(count):
        scaled = [lower[j, k] * pivot[k] for k in range(j)]
        value = entry[j, j]
        for k in range(j):
            value = value - lower[j, k] * scaled[k]
        pivot.append(value)
        for i in range(j + 1, count):
            value = entry[i, j]
            for k in range(j):
                value = value - lower[i, k] * scaled[k]
            lower[i, j] = value / pivot[j]
    middle = []
    for i in range(count):
        value = jnp.ones_like(pivot[0])
        for k in range(i):
            value = value - lower[i, k] * middle[k]
        middle.append(value)
    solved = [None] * count
    for i in reversed(range(count)):
        value = middle[i] / pivot[i]
        for k in range(i + 1, count):
            value = value - lower[k, i] * solved[k]
        solved[i] = value
    total = solved[0]
    for value in solved[1:]:
        total = total + value
    return [value / total for value in solved]


def mix_kernel(
    slabs, pencils, cells, slots,
    live_ref, res_hbm, dens_hbm, occ_hbm, occ_res_hbm, species_hbm, corner_hbm,
    xf_hbm, yt_hbm, zf_hbm, zb_hbm, xb_hbm,
    out_ref, occ_out_ref, last,
    res, dens, occ_ref, occ_res_ref, species_ref, corner_ref,
    first_turn, sums, send_box, land_box, planes, spectrum, back_box, field,
    xf_ref, yt_ref, zf_ref, zb_ref, xb_ref,
    res_sem, table_sem, sum_sem, go_send, go_recv, back_send, back_recv,
):
    devices = slabs * pencils
    count, z_local, y_local, x_length = res.shape
    slots_k = x_length // 2 // devices
    freqs = 2 * slots_k
    z_length = z_local * slabs
    y_length = y_local * pencils
    tiles_out = send_box.shape[0]
    slab = lax.axis_index("slab")
    pencil = lax.axis_index("pencil")
    me = slab * pencils + pencil
    pairs = pairs_of(count)
    ends = cuts_of(slots_k)
    chunks = list(zip([0] + ends[:-1], ends))

    def place(index):
        return (lax.div(index, pencils), lax.rem(index, pencils))

    def other(step):
        return lax.rem(me + step, devices)

    sources = (
        occ_res_hbm, species_hbm, corner_hbm, xf_hbm,
        occ_hbm, dens_hbm, yt_hbm, zf_hbm, zb_hbm, xb_hbm,
    )
    targets = (
        occ_res_ref, species_ref, corner_ref, xf_ref,
        occ_ref, dens, yt_ref, zf_ref, zb_ref, xb_ref,
    )
    loads = [
        pltpu.make_async_copy(a, b, table_sem.at[at])
        for at, (a, b) in enumerate(zip(sources, targets))
    ]

    def res_load(z):
        return pltpu.make_async_copy(res_hbm.at[:, z], res.at[:, z], res_sem.at[z])

    res_loads = [res_load(z) for z in range(z_local)]
    for copy in loads[1:3] + res_loads + loads[:1] + loads[3:4]:
        copy.start()

    barrier = pltpu.get_barrier_semaphore()

    def greet(step, _):
        pl.semaphore_signal(
            barrier, inc=1, device_id=place(other(step)), device_id_type=MESH
        )
        return 0

    lax.fori_loop(1, devices, greet, 0)

    def wide(value):
        width = value.shape[1]
        if width == 128:
            return value
        return jnp.concatenate((value, jnp.zeros((8, 128 - width), value.dtype)), axis=1)

    def lanes_of(length):
        return [(at, min(at + 128, length)) for at in range(0, length, 128)]

    def plane(z, acc):
        acc = list(acc)
        res_load(z).wait()
        for row in range(0, y_local, 8):
            for start, stop in lanes_of(x_length):
                part = [wide(res[i, z, row:row + 8, start:stop]) for i in range(count)]
                for at, (i, j) in enumerate(pairs):
                    acc[at] = acc[at] + part[i] * part[j]
        return tuple(acc)

    nothing = tuple(jnp.zeros((8, 128), jnp.float32) for _ in pairs)
    acc = lax.fori_loop(0, z_local, plane, nothing)

    for copy in loads[:3]:
        copy.wait()
    slot_count, entries = occ_ref.shape[1:]
    species = species_ref[...]
    orbitals = jnp.zeros_like(species)
    for species_index, orbital_number in enumerate(species_orbitals):
        orbitals = jnp.where(species == species_index, orbital_number, orbitals)
    square = (slot_count, slot_count)
    row_index = lax.broadcasted_iota(jnp.int32, square, 0)
    column_index = lax.broadcasted_iota(jnp.int32, square, 1)
    chosen = (row_index == column_index) & (column_index < live_ref[0])
    limit = jnp.sum(
        jnp.where(chosen, orbitals.astype(jnp.float32), 0.0), axis=1, keepdims=True
    )
    mask = (corner_ref[...] < limit).astype(jnp.float32)
    ratio = cells / (100.0 * slots)
    blocks_acc = [jnp.zeros((8, 128), jnp.float32) for _ in pairs]
    for first in range(0, slot_count, 8):
        for start, stop in lanes_of(entries):
            part = [
                wide(occ_res_ref[i, first:first + 8, start:stop] * mask[first:first + 8, start:stop])
                for i in range(count)
            ]
            for at, (i, j) in enumerate(pairs):
                blocks_acc[at] = blocks_acc[at] + part[i] * part[j]
    acc = [value + blocks * ratio for value, blocks in zip(acc, blocks_acc)]
    for copy in loads[4:]:
        copy.start()
    stacked = jnp.concatenate([jnp.sum(a, axis=0, keepdims=True) for a in acc], axis=0)
    totals = jnp.sum(stacked, axis=1, keepdims=True) / cells
    shape = (len(pairs), 128)
    pair_index = lax.broadcasted_iota(jnp.int32, shape, 0)
    across = lax.broadcasted_iota(jnp.int32, shape, 1)
    packed = jnp.sum(jnp.where(pair_index == across, totals, 0.0), axis=0, keepdims=True)
    sums[pl.ds(me, 1), :] = packed

    pl.semaphore_wait(barrier, devices - 1)

    def sum_copy(source, target):
        return pltpu.make_async_remote_copy(
            src_ref=sums.at[pl.ds(source, 1)], dst_ref=sums.at[pl.ds(source, 1)],
            send_sem=sum_sem.at[0], recv_sem=sum_sem.at[1],
            device_id=place(target), device_id_type=MESH,
        )

    def start_sum(step, _):
        sum_copy(me, other(step)).start()
        return 0

    lax.fori_loop(1, devices, start_sum, 0)
    all_sums = pltpu.make_async_remote_copy(
        src_ref=sums.at[pl.ds(0, devices - 1)], dst_ref=sums.at[pl.ds(0, devices - 1)],
        send_sem=sum_sem.at[0], recv_sem=sum_sem.at[1],
        device_id=place(other(1)), device_id_type=MESH,
    )

    loads[3].wait()
    opening = slice(0, 2 * ends[0] * devices)

    left = (xf_ref[0, opening, :], xf_ref[1, opening, :])
    for i in range(count):
        history = split(res[i].reshape(z_local * y_local, x_length))
        first_turn[i] = three(left, history, ((1,), (1,)))

    all_sums.wait_recv()
    gathered = jnp.sum(sums[...], axis=0, keepdims=True)
    lane_index = lax.broadcasted_iota(jnp.int32, (1, 128), 1)
    entry = {
        pair: jnp.sum(jnp.where(lane_index == at, gathered, 0.0), axis=1, keepdims=True)
        for at, pair in enumerate(pairs)
    }
    weights = solve_weights(entry, count)

    def share(chunk, index):
        first, end = chunks[chunk]
        size = 2 * (end - first)
        return pl.ds(2 * first * devices + index * size, size)

    def go_copy(chunk, source, target):
        return pltpu.make_async_remote_copy(
            src_ref=send_box.at[:, share(chunk, target), :],
            dst_ref=land_box.at[:, share(chunk, source), :],
            send_sem=go_send.at[0], recv_sem=go_recv.at[chunk],
            device_id=place(target), device_id_type=MESH,
        )

    def landing(chunk, rows):
        if chunk < len(chunks) - 1:
            return field.at[:, rows, :]
        return last.at[:, pl.ds(rows.start - 2 * chunks[chunk][0] * devices, rows.size), :]

    def back_copy(chunk, source, target):
        return pltpu.make_async_remote_copy(
            src_ref=back_box.at[:, share(chunk, target), :],
            dst_ref=landing(chunk, share(chunk, source)),
            send_sem=back_send.at[0], recv_sem=back_recv.at[chunk],
            device_id=place(target), device_id_type=MESH,
        )

    def start_all(copy, chunk):
        def start(step, _):
            copy(chunk, me, other(step)).start()
            return 0

        lax.fori_loop(1, devices, start, 0)

    def whole(source, target, rows, send, recv):
        return pltpu.make_async_remote_copy(
            src_ref=source.at[:, rows, :], dst_ref=target.at[:, rows, :],
            send_sem=send, recv_sem=recv, device_id=place(other(1)), device_id_type=MESH,
        )

    def land_all(source, target, send, recv, chunk):
        first, end = chunks[chunk]
        rows = pl.ds(2 * first * devices, 2 * (end - first) * (devices - 1))
        whole(source, target, rows, send.at[0], recv.at[chunk]).wait_recv()

    def drain_all(source, target, send, recv):
        rows = pl.ds(0, freqs * (devices - 1))
        whole(source, target, rows, send.at[0], recv.at[0]).wait_send()

    def mixed(parts):
        total = weights[0] * parts[0]
        for i in range(1, count):
            total = total + weights[i] * parts[i]
        return total

    turned = mixed([first_turn[i] for i in range(count)])
    for t in range(tiles_out):
        send_box[t, opening, :] = turned[:, t * 128:(t + 1) * 128]
    start_all(go_copy, 0)
    land_box[:, share(0, me), :] = send_box[:, share(0, me), :]

    mixture = [mixed([res[i, z] for i in range(count)]) for z in range(z_local)]
    mixture = split(jnp.concatenate(mixture, axis=0))
    for chunk, (first, end) in enumerate(chunks):
        if chunk == 0:
            continue
        rows = slice(2 * first * devices, 2 * end * devices)
        turned = three((xf_ref[0, rows, :], xf_ref[1, rows, :]), mixture, ((1,), (1,)))
        for t in range(tiles_out):
            send_box[t, rows, :] = turned[:, t * 128:(t + 1) * 128]
        start_all(go_copy, chunk)
        land_box[:, share(chunk, me), :] = send_box[:, share(chunk, me), :]

    for copy in loads[4:]:
        copy.wait()
    for z in range(z_local):
        out_ref[z * y_local:(z + 1) * y_local, :] = mixed([dens[i, z] for i in range(count)])
    occ_out_ref[...] = mask * mixed(
        [occ_ref[i] + block_mixing * occ_res_ref[i] for i in range(count)]
    )
    all_sums.wait_send()

    z_forward = (zf_ref[0], zf_ref[1])
    z_back = (zb_ref[0], zb_ref[1])
    y_cosine = (yt_ref[0, 0], yt_ref[1, 0])
    y_sine = (yt_ref[0, 1], yt_ref[1, 1])
    shape = (2 * z_length, y_length)
    z_index = lax.rem(lax.broadcasted_iota(jnp.int32, shape, 0), z_length)
    y_index = lax.broadcasted_iota(jnp.int32, shape, 1)
    z_size = jnp.minimum(z_index, z_length - z_index).astype(jnp.float32)
    y_size = jnp.minimum(y_index, y_length - y_index).astype(jnp.float32)
    flat = z_size * z_size + y_size * y_size

    def filtered(wave, freq_x):
        size = freq_x.astype(jnp.float32)
        square = flat + size * size
        return split(wave * (square / (square + kerker_wave * kerker_wave)))

    for chunk, (first, end) in enumerate(chunks):
        size = 2 * (end - first)
        base = 2 * first * devices
        land_all(send_box, land_box, go_send, go_recv, chunk)
        for p in range(pencils):
            for f in range(size):
                joined = jnp.concatenate(
                    [
                        land_box[t, pl.ds(base + p * size + f, slabs, stride=pencils * size), :]
                        for t in range(tiles_out)
                    ],
                    axis=1,
                )
                for z in range(z_local):
                    planes[
                        2 * first + f, z * slabs:(z + 1) * slabs, p * y_local:(p + 1) * y_local
                    ] = joined[:, z * y_local:(z + 1) * y_local]
        block = split(planes[2 * first:2 * end].reshape(size * z_length, y_length))
        along_cosine = three(block, y_cosine, ((1,), (0,)))
        along_sine = three(block, y_sine, ((1,), (0,)))
        extra = first == 0
        for k in range(first, end):
            top, low = 2 * (k - first) * z_length, (2 * (k - first) + 1) * z_length
            stop = low + z_length
            real = along_cosine[top:low] + along_sine[low:stop]
            imag = along_cosine[low:stop] - along_sine[top:low]
            wave = three(z_forward, split(jnp.concatenate((real, imag), axis=0)), ((1,), (0,)))
            freq_x = me * slots_k + k
            spectrum[k - first] = three(z_back, filtered(wave, freq_x), ((1,), (0,)))
            if k == 0:
                freq_x = jnp.where(me == 0, x_length // 2, freq_x)
                spectrum[end] = three(z_back, filtered(wave, freq_x), ((1,), (0,)))
        used = end - first + (1 if extra else 0)
        block = split(spectrum[0:used].reshape(used * 2 * z_length, y_length))
        along_cosine = three(block, y_cosine, ((1,), (0,)))
        along_sine = three(block, y_sine, ((1,), (0,)))
        for k in range(first, end):
            top, low = 2 * (k - first) * z_length, (2 * (k - first) + 1) * z_length
            stop = low + z_length
            real = along_cosine[top:low] - along_sine[low:stop]
            if k == 0:
                top, low = 2 * end * z_length, (2 * end + 1) * z_length
                stop = low + z_length
            imag = along_cosine[low:stop] + along_sine[top:low]
            for c, part in enumerate((real, imag)):
                for p in range(pencils):
                    joined = jnp.concatenate(
                        [
                            part[z * slabs:(z + 1) * slabs, p * y_local:(p + 1) * y_local]
                            for z in range(z_local)
                        ],
                        axis=1,
                    )
                    start = base + p * size + 2 * (k - first) + c
                    for t in range(tiles_out):
                        back_box[t, pl.ds(start, slabs, stride=pencils * size), :] = joined[
                            :, t * 128:(t + 1) * 128
                        ]
        start_all(back_copy, chunk)
        landing(chunk, share(chunk, me))[...] = back_box[:, share(chunk, me), :]

    drain_all(send_box, land_box, go_send, go_recv)
    for chunk, (first, end) in enumerate(chunks):
        rows = pl.ds(2 * first * devices, 2 * (end - first) * (devices - 1))
        pltpu.make_async_remote_copy(
            src_ref=back_box.at[:, rows, :], dst_ref=landing(chunk, rows),
            send_sem=back_send.at[0], recv_sem=back_recv.at[chunk],
            device_id=place(other(1)), device_id_type=MESH,
        ).wait_recv()
        if chunk == len(chunks) - 1:
            continue
        used = slice(2 * first * devices, 2 * end * devices)
        table = (xb_ref[0, used, :], xb_ref[1, used, :])
        for t in range(tiles_out):
            rows = slice(t * 128, (t + 1) * 128)
            out_ref[rows, :] = out_ref[rows, :] + three(
                split(field[t, used, :]), table, ((0,), (0,))
            )
    drain_all(back_box, back_box, back_send, back_recv)


def finish_kernel(last, dens_ref, occ_ref, xb_ref, out_hbm, occ_hbm, out_ref, sem):
    tiles = last.shape[0]
    table = (xb_ref[0], xb_ref[1])
    copies = [pltpu.make_async_copy(occ_ref, occ_hbm, sem.at[tiles])]
    copies[0].start()
    for t in range(tiles):
        rows = slice(t * 128, (t + 1) * 128)
        out_ref[rows, :] = dens_ref[rows, :] + three(split(last[t]), table, ((0,), (0,)))
        copies.append(pltpu.make_async_copy(out_ref.at[rows], out_hbm.at[rows], sem.at[t]))
        copies[-1].start()
    for copy in copies:
        copy.wait()


def fused_body(
    density_history, residual_history, occupancy_history, occupancy_residual, species, slot_count
):
    count, z_local, y_local, x_length = residual_history.shape
    slabs = lax.axis_size("slab")
    pencils = lax.axis_size("pencil")
    devices = slabs * pencils
    z_length, y_length = z_local * slabs, y_local * pencils
    freqs = x_length // devices
    entry = np.arange(ORBITALS * ORBITALS)
    corner = np.maximum(entry // ORBITALS, entry % ORBITALS)[None].astype(np.float32)
    x_forward, x_back, *others = tables(x_length, y_length, z_length, pencils, slabs)
    constants = [x_forward, *others, x_back]
    ends = cuts_of(freqs // 2)
    chunks = len(ends)
    late = 2 * ends[-2] * devices if chunks > 1 else 0
    constants[-1] = x_back[:, :late] if late else x_back[:, :16]
    constants = [jnp.asarray(t) for t in constants]
    vmem = pl.BlockSpec(memory_space=pltpu.VMEM)
    hbm = pl.BlockSpec(memory_space=pltpu.HBM)
    box = (z_local * y_local // 128, devices * freqs, 128)
    sems = pltpu.SemaphoreType.DMA
    flat = jax.ShapeDtypeStruct((z_local * y_local, x_length), jnp.float32)
    blocks = jax.ShapeDtypeStruct(occupancy_history.shape[1:], jnp.float32)
    smalls = [
        occupancy_history, occupancy_residual, species[None], jnp.asarray(corner)
    ]
    mixed, mixed_blocks, last = pl.pallas_call(
        functools.partial(
            mix_kernel, slabs, pencils,
            z_length * y_length * x_length, species.shape[0] * devices,
        ),
        out_shape=(flat, blocks, jax.ShapeDtypeStruct((box[0], box[1] - late, 128), jnp.float32)),
        in_specs=[pl.BlockSpec(memory_space=pltpu.SMEM)] + [hbm] * (6 + len(constants)),
        out_specs=(vmem, vmem, vmem),
        scratch_shapes=[
            pltpu.VMEM(residual_history.shape, jnp.float32),
            pltpu.VMEM(residual_history.shape, jnp.float32),
            *[pltpu.VMEM(t.shape, t.dtype) for t in smalls],
            pltpu.VMEM((count, 2 * ends[0] * devices, z_local * y_local), jnp.float32),
            pltpu.VMEM((devices, 128), jnp.float32),
            pltpu.VMEM(box, jnp.float32),
            pltpu.VMEM(box, jnp.float32),
            pltpu.VMEM((freqs, z_length, y_length), jnp.float32),
            pltpu.VMEM((freqs // 2 + 1, 2 * z_length, y_length), jnp.float32),
            pltpu.VMEM(box, jnp.float32),
            pltpu.VMEM((box[0], late or 16, 128), jnp.float32),
            *[pltpu.VMEM(t.shape, t.dtype) for t in constants],
            sems((z_local,)),
            sems((5 + len(constants),)),
            sems((2,)),
            sems((1,)), sems((chunks,)),
            sems((1,)), sems((chunks,)),
        ],
        compiler_params=pltpu.CompilerParams(
            collective_id=0, has_side_effects=True, vmem_limit_bytes=VMEM_LIMIT
        ),
    )(slot_count, *[
        pltpu.with_memory_space_constraint(value, pltpu.HBM)
        for value in (residual_history, density_history, *smalls, *constants)
    ])
    tiles = box[0]
    new_density, new_blocks = pl.pallas_call(
        finish_kernel,
        out_shape=(flat, blocks),
        in_specs=[vmem] * 4,
        out_specs=(hbm, hbm),
        scratch_shapes=[pltpu.VMEM(flat.shape, flat.dtype), sems((tiles + 1,))],
        compiler_params=pltpu.CompilerParams(vmem_limit_bytes=8 * 1024 * 1024),
    )(last, mixed, mixed_blocks, jnp.asarray(x_back[:, late:]))
    return new_density.reshape(z_local, y_local, x_length), new_blocks


def solution(mesh):
    placed = (
        P(None, "slab", "pencil", None),
        P(None, "slab", "pencil", None),
        P(None, ("slab", "pencil"), None),
        P(None, ("slab", "pencil"), None),
        P(("slab", "pencil")),
        P(("slab", "pencil")),
    )
    devices = mesh.shape["slab"] * mesh.shape["pencil"]

    def chosen(*arrays):
        x_length = arrays[0].shape[3]
        _, z_local, y_local, _ = arrays[0].shape
        fits = (
            x_length % (2 * devices) == 0
            and mesh.shape["slab"] % 8 == 0
            and y_local % 16 == 0
            and z_local * y_local % 128 == 0
        )
        return (fused_body if fits else body)(*arrays)

    return jax.shard_map(
        chosen,
        mesh=mesh,
        in_specs=placed,
        out_specs=(P("slab", "pencil", None), P(("slab", "pencil"), None)),
        check_vma=False,
    )
```

```python
import functools
import math

import jax
import jax.numpy as jnp
import numpy as np
from jax import lax
from jax.experimental import pallas as pl
from jax.experimental.pallas import tpu as pltpu
from jax.sharding import PartitionSpec as P

ORBITALS = 18


highest = lax.Precision.HIGHEST
grid_mixing = 0.5
block_mixing = 0.5
kerker_wave = 6.0
species_orbitals = (18, 13, 8, 5)


def block_mask(species, slot_count):
    live = jnp.arange(species.shape[0], dtype=jnp.int32) < slot_count[0]
    orbitals = jnp.zeros_like(species)
    for species_index, orbital_number in enumerate(species_orbitals):
        orbitals = orbitals + orbital_number * (species == species_index).astype(jnp.int32)
    entry = jnp.arange(ORBITALS * ORBITALS, dtype=jnp.int32)
    row_index = entry // ORBITALS
    column_index = entry % ORBITALS
    inside = (
        (row_index[None, :] < orbitals[:, None])
        & (column_index[None, :] < orbitals[:, None])
        & live[:, None]
    )
    return inside.astype(jnp.float32)


def mixing_weights(intersection):
    factor = jnp.linalg.cholesky(intersection)
    column = jnp.ones((intersection.shape[0], 1), intersection.dtype)
    middle = lax.linalg.triangular_solve(factor, column, left_side=True, lower=True)
    solved = lax.linalg.triangular_solve(
        factor, middle, left_side=True, lower=True, transpose_a=True
    )
    return solved[:, 0] / jnp.sum(solved)


def cosine_sine(length, freq_index, space_index):
    product = freq_index * space_index % length
    angle = 2.0 * math.pi / length * product.astype(jnp.float32)
    return (jnp.cos(angle), jnp.sin(angle))


def forward_spectra(fields, pencil_move, slab_move):
    batches, z_local, y_local, x_length = fields.shape
    pencil_count = lax.axis_size("pencil")
    slab_count = lax.axis_size("slab")
    x_columns = x_length // 2
    kx_local = x_columns // pencil_count
    y_length = y_local * pencil_count
    ky_local = y_length // slab_count
    z_length = z_local * slab_count
    freq_index = jnp.arange(x_columns, dtype=jnp.int32).reshape(pencil_count, kx_local, 1)
    space_index = jnp.arange(x_length, dtype=jnp.int32).reshape(1, 1, x_length)
    cosine, sine = cosine_sine(x_length, freq_index, space_index)
    nyquist = cosine_sine(x_length, jnp.full((1, 1, 1), x_length // 2, jnp.int32), space_index)[0]
    sine = jnp.where(freq_index == 0, -nyquist, sine)
    real_part = jnp.einsum("bzyx,pkx->bpkzy", fields, cosine, precision=highest)
    imag_part = -jnp.einsum("bzyx,pkx->bpkzy", fields, sine, precision=highest)
    packed = jnp.stack((real_part, imag_part), axis=1).reshape(batches, 2, pencil_count, -1)
    moved = pencil_move(packed).reshape(batches, 2, pencil_count, kx_local, z_local, y_local)
    freq_index = jnp.arange(y_length, dtype=jnp.int32).reshape(slab_count, ky_local, 1, 1)
    space_index = jnp.arange(y_length, dtype=jnp.int32).reshape(1, 1, pencil_count, y_local)
    cosine, sine = cosine_sine(y_length, freq_index, space_index)
    real_input = moved[:, 0]
    imag_input = moved[:, 1]
    form = "bskzy,glsy->bgklz"
    real_part = jnp.einsum(form, real_input, cosine, precision=highest) + jnp.einsum(
        form, imag_input, sine, precision=highest
    )
    imag_part = jnp.einsum(form, imag_input, cosine, precision=highest) - jnp.einsum(
        form, real_input, sine, precision=highest
    )
    packed = jnp.stack((real_part, imag_part), axis=1).reshape(batches, 2, slab_count, -1)
    moved = slab_move(packed).reshape(batches, 2, slab_count, kx_local, ky_local, z_local)
    freq_index = jnp.arange(z_length, dtype=jnp.int32).reshape(z_length, 1, 1)
    space_index = jnp.arange(z_length, dtype=jnp.int32).reshape(1, slab_count, z_local)
    cosine, sine = cosine_sine(z_length, freq_index, space_index)
    real_input = moved[:, 0]
    imag_input = moved[:, 1]
    form = "bgklz,mgz->bklm"
    real_part = jnp.einsum(form, real_input, cosine, precision=highest) + jnp.einsum(
        form, imag_input, sine, precision=highest
    )
    imag_part = jnp.einsum(form, imag_input, cosine, precision=highest) - jnp.einsum(
        form, real_input, sine, precision=highest
    )
    return jnp.stack((real_part, imag_part), axis=1)


def magnitude(index, length):
    return jnp.minimum(index, length - index).astype(jnp.float32)


def kerker_factor(freq_x, ky_local, x_length, y_length, z_length):
    freq_y = lax.axis_index("slab") * ky_local + jnp.arange(ky_local, dtype=jnp.int32)
    freq_z = jnp.arange(z_length, dtype=jnp.int32)
    square = (
        magnitude(freq_x, x_length)[:, None, None] ** 2
        + magnitude(freq_y, y_length)[None, :, None] ** 2
        + magnitude(freq_z, z_length)[None, None, :] ** 2
    )
    return square / (square + kerker_wave * kerker_wave)


def inverse_field(spectrum, z_local, y_local, x_length):
    pencil_count = lax.axis_size("pencil")
    slab_count = lax.axis_size("slab")
    x_columns = x_length // 2
    kx_local = x_columns // pencil_count
    slots = spectrum.shape[1]
    y_length = y_local * pencil_count
    ky_local = y_length // slab_count
    z_length = z_local * slab_count
    freq_index = jnp.arange(z_length, dtype=jnp.int32).reshape(z_length, 1, 1)
    space_index = jnp.arange(z_length, dtype=jnp.int32).reshape(1, slab_count, z_local)
    cosine, sine = cosine_sine(z_length, freq_index, space_index)
    real_input = spectrum[0]
    imag_input = spectrum[1]
    form = "klm,mdz->dklz"
    real_part = jnp.einsum(form, real_input, cosine, precision=highest) - jnp.einsum(
        form, imag_input, sine, precision=highest
    )
    imag_part = jnp.einsum(form, real_input, sine, precision=highest) + jnp.einsum(
        form, imag_input, cosine, precision=highest
    )
    packed = jnp.stack((real_part, imag_part), axis=0).reshape(2, slab_count, -1)
    moved = lax.all_to_all(packed, "slab", split_axis=1, concat_axis=1, tiled=True).reshape(
        2, slab_count, slots, ky_local, z_local
    )
    freq_index = jnp.arange(y_length, dtype=jnp.int32).reshape(slab_count, ky_local, 1, 1)
    space_index = jnp.arange(y_length, dtype=jnp.int32).reshape(1, 1, pencil_count, y_local)
    cosine, sine = cosine_sine(y_length, freq_index, space_index)
    real_input = moved[0]
    imag_input = moved[1]
    form = "gklz,glqy->qkzy"
    real_part = jnp.einsum(form, real_input, cosine, precision=highest) - jnp.einsum(
        form, imag_input, sine, precision=highest
    )
    imag_part = jnp.einsum(form, real_input, sine, precision=highest) + jnp.einsum(
        form, imag_input, cosine, precision=highest
    )
    packed = jnp.stack((real_part, imag_part), axis=0).reshape(2, pencil_count, -1)
    moved = lax.all_to_all(packed, "pencil", split_axis=1, concat_axis=1, tiled=True).reshape(
        2, pencil_count, slots, z_local, y_local
    )
    pencil_index = jnp.arange(pencil_count, dtype=jnp.int32).reshape(pencil_count, 1, 1)
    slot_index = jnp.arange(slots, dtype=jnp.int32).reshape(1, slots, 1)
    space_index = jnp.arange(x_length, dtype=jnp.int32).reshape(1, 1, x_length)
    freq_index = pencil_index * kx_local + slot_index
    cosine, sine = cosine_sine(x_length, freq_index, space_index)
    nyquist = cosine_sine(x_length, jnp.full((1, 1, 1), x_length // 2, jnp.int32), space_index)[0]
    ordinary = slot_index < kx_local
    doubling = jnp.where(freq_index == 0, 1.0, 2.0)
    real_table = jnp.where(ordinary, doubling * cosine, 0.0)
    imag_table = jnp.where(ordinary, -doubling * sine, jnp.where(pencil_index == 0, nyquist, 0.0))
    form = "pkzy,pkx->zyx"
    field = jnp.einsum(form, moved[0], real_table, precision=highest) + jnp.einsum(
        form, moved[1], imag_table, precision=highest
    )
    return field / (x_length * y_length * z_length)


def body(
    density_history, residual_history, occupancy_history, occupancy_residual, species, slot_count
):
    histories, z_local, y_local, x_length = residual_history.shape
    slab_count = lax.axis_size("slab")
    pencil_count = lax.axis_size("pencil")
    cell_total = z_local * slab_count * y_local * pencil_count * x_length
    slot_total = species.shape[0] * slab_count * pencil_count
    mask = block_mask(species, slot_count)
    flat = residual_history.reshape(histories, -1)
    grid_local = jnp.dot(flat, flat.T, precision=highest) / cell_total
    blocks = (occupancy_residual * mask[None]).reshape(histories, -1)
    block_local = jnp.dot(blocks, blocks.T, precision=highest) / (100.0 * slot_total)
    grid_intersection, block_intersection = lax.psum((grid_local, block_local), ("slab", "pencil"))
    weights = mixing_weights(grid_intersection + block_intersection)
    mixed = jnp.tensordot(weights, residual_history, axes=1, precision=highest)
    spectrum = forward_spectra(
        mixed[None],
        lambda packed: lax.all_to_all(packed, "pencil", split_axis=2, concat_axis=2, tiled=True),
        lambda packed: lax.all_to_all(packed, "slab", split_axis=2, concat_axis=2, tiled=True),
    )[0]
    x_columns = x_length // 2
    kx_local = x_columns // pencil_count
    y_length = y_local * pencil_count
    z_length = z_local * slab_count
    ky_local = y_length // slab_count
    freq_x = lax.axis_index("pencil") * kx_local + jnp.arange(kx_local, dtype=jnp.int32)
    factor = kerker_factor(freq_x, ky_local, x_length, y_length, z_length)
    filtered_spectrum = spectrum * factor[None]
    nyquist_x = jnp.full((1,), x_length // 2, jnp.int32)
    nyquist_factor = kerker_factor(nyquist_x, ky_local, x_length, y_length, z_length)
    owner = (lax.axis_index("pencil") == 0).astype(jnp.float32)
    extra = spectrum[:, 0:1] * nyquist_factor[None] * owner
    filtered_spectrum = jnp.concatenate((filtered_spectrum, extra), axis=1)
    filtered = inverse_field(filtered_spectrum, z_local, y_local, x_length)
    new_density = (
        jnp.tensordot(weights, density_history, axes=1, precision=highest) + grid_mixing * filtered
    )
    mixed_blocks = jnp.tensordot(
        weights, occupancy_history + block_mixing * occupancy_residual, axes=1, precision=highest
    )
    return (new_density, mask * mixed_blocks)


MESH = pl.DeviceIdType.MESH
VMEM_LIMIT = 40000 * 1024


def split(value):
    high = value.astype(jnp.bfloat16)
    low = (value - high.astype(jnp.float32)).astype(jnp.bfloat16)
    return high, low


def three(left, right, dims):
    numbers = (dims, ((), ()))
    dot = functools.partial(
        lax.dot_general, dimension_numbers=numbers, preferred_element_type=jnp.float32
    )
    return dot(left[1], right[0]) + dot(left[0], right[1]) + dot(left[0], right[0])


def halves(table):
    table = np.asarray(table, np.float32)
    high = table.astype(jnp.bfloat16)
    low = (table - high.astype(np.float32)).astype(jnp.bfloat16)
    return np.stack((high, low))


def waves(rows, columns, length):
    angle = 2.0 * np.pi / length * (np.outer(rows, columns) % length)
    return np.cos(angle), np.sin(angle)


def tables(x_length, y_length, z_length, pencil_count, slab_count):
    columns = x_length // 2
    cosine, sine = waves(np.arange(columns), np.arange(x_length), x_length)
    nyquist = np.where(np.arange(x_length) % 2 == 0, 1.0, -1.0)
    imag = -sine
    imag[0] = nyquist
    slots_k = columns // (pencil_count * slab_count)
    owner, slot = np.arange(columns) // slots_k, np.arange(columns) % slots_k
    chunk = np.searchsorted(cuts_of(slots_k), slot, side="right")
    order = np.lexsort((slot, owner, chunk))
    x_forward = np.stack((cosine, imag), axis=1)[order].reshape(x_length, x_length)
    doubling = np.where(np.arange(columns) == 0, 1.0, 2.0)[:, None]
    back = np.stack((doubling * cosine, doubling * imag), axis=1)[order]
    back = back.reshape(x_length, x_length)
    x_back = back * (grid_mixing / (x_length * y_length * z_length))
    cosine, sine = waves(np.arange(y_length), np.arange(y_length), y_length)
    along_y = np.stack((cosine, sine))
    cosine, sine = waves(np.arange(z_length), np.arange(z_length), z_length)
    order = np.arange(z_length).reshape(slab_count, -1).T.reshape(-1)
    cosine, sine = cosine[:, order], sine[:, order]
    z_forward = np.block([[cosine, sine], [-sine, cosine]])
    z_back = np.block([[cosine.T, -sine.T], [sine.T, cosine.T]])
    return [halves(t) for t in (x_forward, x_back, along_y, z_forward, z_back)]


def cuts_of(slots):
    return [at for at in range(1, slots, 2)] + [slots]


def pairs_of(count):
    return [(i, j) for i in range(count) for j in range(i + 1)]


def solve_weights(entry, count):
    lower, pivot = {}, []
    for j in range(count):
        scaled = [lower[j, k] * pivot[k] for k in range(j)]
        value = entry[j, j]
        for k in range(j):
            value = value - lower[j, k] * scaled[k]
        pivot.append(value)
        for i in range(j + 1, count):
            value = entry[i, j]
            for k in range(j):
                value = value - lower[i, k] * scaled[k]
            lower[i, j] = value / pivot[j]
    middle = []
    for i in range(count):
        value = jnp.ones_like(pivot[0])
        for k in range(i):
            value = value - lower[i, k] * middle[k]
        middle.append(value)
    solved = [None] * count
    for i in reversed(range(count)):
        value = middle[i] / pivot[i]
        for k in range(i + 1, count):
            value = value - lower[k, i] * solved[k]
        solved[i] = value
    total = solved[0]
    for value in solved[1:]:
        total = total + value
    return [value / total for value in solved]


def mix_kernel(
    slabs, pencils, cells, slots,
    live_ref, res_hbm, dens_hbm, occ_hbm, occ_res_hbm, species_hbm, corner_hbm,
    xf_hbm, yt_hbm, zf_hbm, zb_hbm, xb_hbm,
    out_ref, occ_out_ref, last,
    res, dens, occ_ref, occ_res_ref, species_ref, corner_ref,
    first_turn, sums, send_box, land_box, planes, spectrum, back_box, field,
    xf_ref, yt_ref, zf_ref, zb_ref, xb_ref,
    res_sem, table_sem, sum_sem, go_send, go_recv, back_send, back_recv,
):
    devices = slabs * pencils
    count, z_local, y_local, x_length = res.shape
    slots_k = x_length // 2 // devices
    freqs = 2 * slots_k
    z_length = z_local * slabs
    y_length = y_local * pencils
    tiles_out = send_box.shape[0]
    slab = lax.axis_index("slab")
    pencil = lax.axis_index("pencil")
    me = slab * pencils + pencil
    pairs = pairs_of(count)
    ends = cuts_of(slots_k)
    chunks = list(zip([0] + ends[:-1], ends))

    partners = []
    for step in range(1, devices):
        across = pencil + step % pencils
        row = lax.rem(slab + step // pencils + lax.div(across, pencils), slabs)
        column = lax.rem(across, pencils)
        partners.append(((row, column), row * pencils + column))

    sources = (
        occ_res_hbm, species_hbm, corner_hbm, xf_hbm,
        occ_hbm, dens_hbm, yt_hbm, zf_hbm, zb_hbm, xb_hbm,
    )
    targets = (
        occ_res_ref, species_ref, corner_ref, xf_ref,
        occ_ref, dens, yt_ref, zf_ref, zb_ref, xb_ref,
    )
    loads = [
        pltpu.make_async_copy(a, b, table_sem.at[at])
        for at, (a, b) in enumerate(zip(sources, targets))
    ]

    def res_load(z):
        return pltpu.make_async_copy(res_hbm.at[:, z], res.at[:, z], res_sem.at[z])

    res_loads = [res_load(z) for z in range(z_local)]
    for copy in loads[1:3] + res_loads[:-1] + loads[:1] + res_loads[-1:] + loads[3:4]:
        copy.start()

    barrier = pltpu.get_barrier_semaphore()

    for spot, _ in partners:
        pl.semaphore_signal(barrier, inc=1, device_id=spot, device_id_type=MESH)

    def wide(value):
        width = value.shape[1]
        if width == 128:
            return value
        return jnp.concatenate((value, jnp.zeros((8, 128 - width), value.dtype)), axis=1)

    def lanes_of(length):
        return [(at, min(at + 128, length)) for at in range(0, length, 128)]

    def plane(z, acc):
        acc = list(acc)
        res_load(z).wait()
        for row in range(0, y_local, 8):
            for start, stop in lanes_of(x_length):
                part = [wide(res[i, z, row:row + 8, start:stop]) for i in range(count)]
                for at, (i, j) in enumerate(pairs):
                    acc[at] = acc[at] + part[i] * part[j]
        return tuple(acc)

    nothing = tuple(jnp.zeros((8, 128), jnp.float32) for _ in pairs)
    acc = lax.fori_loop(0, z_local - 1, plane, nothing)
    for copy in loads[:3]:
        copy.wait()
    slot_count, entries = occ_ref.shape[1:]
    species = species_ref[...]
    orbitals = jnp.zeros_like(species)
    for species_index, orbital_number in enumerate(species_orbitals):
        orbitals = jnp.where(species == species_index, orbital_number, orbitals)
    square = (slot_count, slot_count)
    row_index = lax.broadcasted_iota(jnp.int32, square, 0)
    column_index = lax.broadcasted_iota(jnp.int32, square, 1)
    chosen = (row_index == column_index) & (column_index < live_ref[0])
    limit = jnp.sum(
        jnp.where(chosen, orbitals.astype(jnp.float32), 0.0), axis=1, keepdims=True
    )
    mask = (corner_ref[...] < limit).astype(jnp.float32)
    ratio = cells / (100.0 * slots)
    blocks_acc = [jnp.zeros((8, 128), jnp.float32) for _ in pairs]
    for first in range(0, slot_count, 8):
        for start, stop in lanes_of(entries):
            part = [
                wide(occ_res_ref[i, first:first + 8, start:stop] * mask[first:first + 8, start:stop])
                for i in range(count)
            ]
            for at, (i, j) in enumerate(pairs):
                blocks_acc[at] = blocks_acc[at] + part[i] * part[j]
    acc = [value + blocks * ratio for value, blocks in zip(acc, blocks_acc)]
    acc = plane(z_local - 1, acc)

    for copy in loads[4:]:
        copy.start()
    stacked = jnp.concatenate([jnp.sum(a, axis=0, keepdims=True) for a in acc], axis=0)
    totals = jnp.sum(stacked, axis=1, keepdims=True) / cells
    shape = (len(pairs), 128)
    pair_index = lax.broadcasted_iota(jnp.int32, shape, 0)
    across = lax.broadcasted_iota(jnp.int32, shape, 1)
    packed = jnp.sum(jnp.where(pair_index == across, totals, 0.0), axis=0, keepdims=True)
    sums[pl.ds(me, 1), :] = packed

    pl.semaphore_wait(barrier, devices - 1)

    for spot, _ in partners:
        pltpu.make_async_remote_copy(
            src_ref=sums.at[pl.ds(me, 1)], dst_ref=sums.at[pl.ds(me, 1)],
            send_sem=sum_sem.at[0], recv_sem=sum_sem.at[1],
            device_id=spot, device_id_type=MESH,
        ).start()
    all_sums = pltpu.make_async_remote_copy(
        src_ref=sums.at[pl.ds(0, devices - 1)], dst_ref=sums.at[pl.ds(0, devices - 1)],
        send_sem=sum_sem.at[0], recv_sem=sum_sem.at[1],
        device_id=partners[0][0], device_id_type=MESH,
    )

    loads[3].wait()
    opening = slice(0, 2 * ends[0] * devices)

    left = (xf_ref[0, opening, :], xf_ref[1, opening, :])
    for i in range(count):
        history = split(res[i].reshape(z_local * y_local, x_length))
        first_turn[i] = three(left, history, ((1,), (1,)))

    all_sums.wait_recv()
    gathered = jnp.sum(sums[...], axis=0, keepdims=True)
    lane_index = lax.broadcasted_iota(jnp.int32, (1, 128), 1)
    entry = {
        pair: jnp.sum(jnp.where(lane_index == at, gathered, 0.0), axis=1, keepdims=True)
        for at, pair in enumerate(pairs)
    }
    weights = solve_weights(entry, count)

    def share(chunk, index):
        first, end = chunks[chunk]
        size = 2 * (end - first)
        return pl.ds(2 * first * devices + index * size, size)

    def go_copy(chunk, spot, target):
        return pltpu.make_async_remote_copy(
            src_ref=send_box.at[:, share(chunk, target), :],
            dst_ref=land_box.at[:, share(chunk, me), :],
            send_sem=go_send.at[0], recv_sem=go_recv.at[chunk],
            device_id=spot, device_id_type=MESH,
        )

    def landing(chunk, rows):
        if chunk < len(chunks) - 1:
            return field.at[:, rows, :]
        return last.at[:, pl.ds(rows.start - 2 * chunks[chunk][0] * devices, rows.size), :]

    def back_copy(chunk, spot, target):
        return pltpu.make_async_remote_copy(
            src_ref=back_box.at[:, share(chunk, target), :],
            dst_ref=landing(chunk, share(chunk, me)),
            send_sem=back_send.at[0], recv_sem=back_recv.at[chunk],
            device_id=spot, device_id_type=MESH,
        )

    def start_all(copy, chunk):
        for spot, target in partners:
            copy(chunk, spot, target).start()

    def whole(source, target, rows, send, recv):
        return pltpu.make_async_remote_copy(
            src_ref=source.at[:, rows, :], dst_ref=target.at[:, rows, :],
            send_sem=send, recv_sem=recv, device_id=partners[0][0], device_id_type=MESH,
        )

    def land_all(source, target, send, recv, chunk):
        first, end = chunks[chunk]
        rows = pl.ds(2 * first * devices, 2 * (end - first) * (devices - 1))
        whole(source, target, rows, send.at[0], recv.at[chunk]).wait_recv()

    def drain_all(source, target, send, recv):
        rows = pl.ds(0, freqs * (devices - 1))
        whole(source, target, rows, send.at[0], recv.at[0]).wait_send()

    def mixed(parts):
        total = weights[0] * parts[0]
        for i in range(1, count):
            total = total + weights[i] * parts[i]
        return total

    turned = mixed([first_turn[i] for i in range(count)])
    for t in range(tiles_out):
        send_box[t, opening, :] = turned[:, t * 128:(t + 1) * 128]
    start_all(go_copy, 0)
    land_box[:, share(0, me), :] = send_box[:, share(0, me), :]

    mixture = [mixed([res[i, z] for i in range(count)]) for z in range(z_local)]
    mixture = split(jnp.concatenate(mixture, axis=0))
    for chunk, (first, end) in enumerate(chunks):
        if chunk == 0:
            continue
        rows = slice(2 * first * devices, 2 * end * devices)
        turned = three((xf_ref[0, rows, :], xf_ref[1, rows, :]), mixture, ((1,), (1,)))
        for t in range(tiles_out):
            send_box[t, rows, :] = turned[:, t * 128:(t + 1) * 128]
        start_all(go_copy, chunk)
        land_box[:, share(chunk, me), :] = send_box[:, share(chunk, me), :]

    for copy in loads[4:]:
        copy.wait()
    for z in range(z_local):
        out_ref[z * y_local:(z + 1) * y_local, :] = mixed([dens[i, z] for i in range(count)])
    occ_out_ref[...] = mask * mixed(
        [occ_ref[i] + block_mixing * occ_res_ref[i] for i in range(count)]
    )
    all_sums.wait_send()

    z_forward = (zf_ref[0], zf_ref[1])
    z_back = (zb_ref[0], zb_ref[1])
    y_cosine = (yt_ref[0, 0], yt_ref[1, 0])
    y_sine = (yt_ref[0, 1], yt_ref[1, 1])
    shape = (2 * z_length, y_length)
    z_index = lax.rem(lax.broadcasted_iota(jnp.int32, shape, 0), z_length)
    y_index = lax.broadcasted_iota(jnp.int32, shape, 1)
    z_size = jnp.minimum(z_index, z_length - z_index).astype(jnp.float32)
    y_size = jnp.minimum(y_index, y_length - y_index).astype(jnp.float32)
    flat = z_size * z_size + y_size * y_size

    def filtered(wave, freq_x):
        size = freq_x.astype(jnp.float32)
        square = flat + size * size
        return split(wave * (square / (square + kerker_wave * kerker_wave)))

    for chunk, (first, end) in enumerate(chunks):
        size = 2 * (end - first)
        base = 2 * first * devices
        land_all(send_box, land_box, go_send, go_recv, chunk)
        for p in range(pencils):
            for f in range(size):
                joined = jnp.concatenate(
                    [
                        land_box[t, pl.ds(base + p * size + f, slabs, stride=pencils * size), :]
                        for t in range(tiles_out)
                    ],
                    axis=1,
                )
                for z in range(z_local):
                    planes[
                        2 * first + f, z * slabs:(z + 1) * slabs, p * y_local:(p + 1) * y_local
                    ] = joined[:, z * y_local:(z + 1) * y_local]
        block = split(planes[2 * first:2 * end].reshape(size * z_length, y_length))
        along_cosine = three(block, y_cosine, ((1,), (0,)))
        along_sine = three(block, y_sine, ((1,), (0,)))
        extra = first == 0
        for k in range(first, end):
            top, low = 2 * (k - first) * z_length, (2 * (k - first) + 1) * z_length
            stop = low + z_length
            real = along_cosine[top:low] + along_sine[low:stop]
            imag = along_cosine[low:stop] - along_sine[top:low]
            wave = three(z_forward, split(jnp.concatenate((real, imag), axis=0)), ((1,), (0,)))
            freq_x = me * slots_k + k
            spectrum[k - first] = three(z_back, filtered(wave, freq_x), ((1,), (0,)))
            if k == 0:
                freq_x = jnp.where(me == 0, x_length // 2, freq_x)
                spectrum[end] = three(z_back, filtered(wave, freq_x), ((1,), (0,)))
        used = end - first + (1 if extra else 0)
        block = split(spectrum[0:used].reshape(used * 2 * z_length, y_length))
        along_cosine = three(block, y_cosine, ((1,), (0,)))
        along_sine = three(block, y_sine, ((1,), (0,)))
        for k in range(first, end):
            top, low = 2 * (k - first) * z_length, (2 * (k - first) + 1) * z_length
            stop = low + z_length
            real = along_cosine[top:low] - along_sine[low:stop]
            if k == 0:
                top, low = 2 * end * z_length, (2 * end + 1) * z_length
                stop = low + z_length
            imag = along_cosine[low:stop] + along_sine[top:low]
            for c, part in enumerate((real, imag)):
                for p in range(pencils):
                    joined = jnp.concatenate(
                        [
                            part[z * slabs:(z + 1) * slabs, p * y_local:(p + 1) * y_local]
                            for z in range(z_local)
                        ],
                        axis=1,
                    )
                    start = base + p * size + 2 * (k - first) + c
                    for t in range(tiles_out):
                        back_box[t, pl.ds(start, slabs, stride=pencils * size), :] = joined[
                            :, t * 128:(t + 1) * 128
                        ]
        start_all(back_copy, chunk)
        landing(chunk, share(chunk, me))[...] = back_box[:, share(chunk, me), :]

    drain_all(send_box, land_box, go_send, go_recv)
    for chunk, (first, end) in enumerate(chunks):
        rows = pl.ds(2 * first * devices, 2 * (end - first) * (devices - 1))
        pltpu.make_async_remote_copy(
            src_ref=back_box.at[:, rows, :], dst_ref=landing(chunk, rows),
            send_sem=back_send.at[0], recv_sem=back_recv.at[chunk],
            device_id=partners[0][0], device_id_type=MESH,
        ).wait_recv()
        if chunk == len(chunks) - 1:
            continue
        used = slice(2 * first * devices, 2 * end * devices)
        table = (xb_ref[0, used, :], xb_ref[1, used, :])
        for t in range(tiles_out):
            rows = slice(t * 128, (t + 1) * 128)
            out_ref[rows, :] = out_ref[rows, :] + three(
                split(field[t, used, :]), table, ((0,), (0,))
            )
    drain_all(back_box, back_box, back_send, back_recv)


def finish_kernel(last, dens_ref, occ_ref, xb_ref, out_hbm, occ_hbm, out_ref, sem):
    tiles = last.shape[0]
    table = (xb_ref[0], xb_ref[1])
    copies = [pltpu.make_async_copy(occ_ref, occ_hbm, sem.at[tiles])]
    copies[0].start()
    for t in range(tiles):
        rows = slice(t * 128, (t + 1) * 128)
        out_ref[rows, :] = dens_ref[rows, :] + three(split(last[t]), table, ((0,), (0,)))
        copies.append(pltpu.make_async_copy(out_ref.at[rows], out_hbm.at[rows], sem.at[t]))
        copies[-1].start()
    for copy in copies:
        copy.wait()


def fused_body(
    density_history, residual_history, occupancy_history, occupancy_residual, species, slot_count
):
    count, z_local, y_local, x_length = residual_history.shape
    slabs = lax.axis_size("slab")
    pencils = lax.axis_size("pencil")
    devices = slabs * pencils
    z_length, y_length = z_local * slabs, y_local * pencils
    freqs = x_length // devices
    entry = np.arange(ORBITALS * ORBITALS)
    corner = np.maximum(entry // ORBITALS, entry % ORBITALS)[None].astype(np.float32)
    x_forward, x_back, *others = tables(x_length, y_length, z_length, pencils, slabs)
    constants = [x_forward, *others, x_back]
    ends = cuts_of(freqs // 2)
    chunks = len(ends)
    late = 2 * ends[-2] * devices if chunks > 1 else 0
    constants[-1] = x_back[:, :late] if late else x_back[:, :16]
    constants = [jnp.asarray(t) for t in constants]
    vmem = pl.BlockSpec(memory_space=pltpu.VMEM)
    hbm = pl.BlockSpec(memory_space=pltpu.HBM)
    box = (z_local * y_local // 128, devices * freqs, 128)
    sems = pltpu.SemaphoreType.DMA
    flat = jax.ShapeDtypeStruct((z_local * y_local, x_length), jnp.float32)
    blocks = jax.ShapeDtypeStruct(occupancy_history.shape[1:], jnp.float32)
    smalls = [
        occupancy_history, occupancy_residual, species[None], jnp.asarray(corner)
    ]
    mixed, mixed_blocks, last = pl.pallas_call(
        functools.partial(
            mix_kernel, slabs, pencils,
            z_length * y_length * x_length, species.shape[0] * devices,
        ),
        out_shape=(flat, blocks, jax.ShapeDtypeStruct((box[0], box[1] - late, 128), jnp.float32)),
        in_specs=[pl.BlockSpec(memory_space=pltpu.SMEM)] + [hbm] * (6 + len(constants)),
        out_specs=(vmem, vmem, vmem),
        scratch_shapes=[
            pltpu.VMEM(residual_history.shape, jnp.float32),
            pltpu.VMEM(residual_history.shape, jnp.float32),
            *[pltpu.VMEM(t.shape, t.dtype) for t in smalls],
            pltpu.VMEM((count, 2 * ends[0] * devices, z_local * y_local), jnp.float32),
            pltpu.VMEM((devices, 128), jnp.float32),
            pltpu.VMEM(box, jnp.float32),
            pltpu.VMEM(box, jnp.float32),
            pltpu.VMEM((freqs, z_length, y_length), jnp.float32),
            pltpu.VMEM((freqs // 2 + 1, 2 * z_length, y_length), jnp.float32),
            pltpu.VMEM(box, jnp.float32),
            pltpu.VMEM((box[0], late or 16, 128), jnp.float32),
            *[pltpu.VMEM(t.shape, t.dtype) for t in constants],
            sems((z_local,)),
            sems((5 + len(constants),)),
            sems((2,)),
            sems((1,)), sems((chunks,)),
            sems((1,)), sems((chunks,)),
        ],
        compiler_params=pltpu.CompilerParams(
            collective_id=0, has_side_effects=True, vmem_limit_bytes=VMEM_LIMIT
        ),
    )(slot_count, *[
        pltpu.with_memory_space_constraint(value, pltpu.HBM)
        for value in (residual_history, density_history, *smalls, *constants)
    ])
    tiles = box[0]
    new_density, new_blocks = pl.pallas_call(
        finish_kernel,
        out_shape=(flat, blocks),
        in_specs=[vmem] * 4,
        out_specs=(hbm, hbm),
        scratch_shapes=[pltpu.VMEM(flat.shape, flat.dtype), sems((tiles + 1,))],
        compiler_params=pltpu.CompilerParams(vmem_limit_bytes=8 * 1024 * 1024),
    )(last, mixed, mixed_blocks, jnp.asarray(x_back[:, late:]))
    return new_density.reshape(z_local, y_local, x_length), new_blocks


def solution(mesh):
    placed = (
        P(None, "slab", "pencil", None),
        P(None, "slab", "pencil", None),
        P(None, ("slab", "pencil"), None),
        P(None, ("slab", "pencil"), None),
        P(("slab", "pencil")),
        P(("slab", "pencil")),
    )
    devices = mesh.shape["slab"] * mesh.shape["pencil"]

    def chosen(*arrays):
        x_length = arrays[0].shape[3]
        _, z_local, y_local, _ = arrays[0].shape
        fits = (
            x_length % (2 * devices) == 0
            and mesh.shape["slab"] % 8 == 0
            and y_local % 16 == 0
            and z_local * y_local % 128 == 0
        )
        return (fused_body if fits else body)(*arrays)

    return jax.shard_map(
        chosen,
        mesh=mesh,
        in_specs=placed,
        out_specs=(P("slab", "pencil", None), P(("slab", "pencil"), None)),
        check_vma=False,
    )
```

```python
import functools
import math

import jax
import jax.numpy as jnp
import numpy as np
from jax import lax
from jax.experimental import pallas as pl
from jax.experimental.pallas import tpu as pltpu
from jax.sharding import PartitionSpec as P

ORBITALS = 18


highest = lax.Precision.HIGHEST
grid_mixing = 0.5
block_mixing = 0.5
kerker_wave = 6.0
species_orbitals = (18, 13, 8, 5)


def block_mask(species, slot_count):
    live = jnp.arange(species.shape[0], dtype=jnp.int32) < slot_count[0]
    orbitals = jnp.zeros_like(species)
    for species_index, orbital_number in enumerate(species_orbitals):
        orbitals = orbitals + orbital_number * (species == species_index).astype(jnp.int32)
    entry = jnp.arange(ORBITALS * ORBITALS, dtype=jnp.int32)
    row_index = entry // ORBITALS
    column_index = entry % ORBITALS
    inside = (
        (row_index[None, :] < orbitals[:, None])
        & (column_index[None, :] < orbitals[:, None])
        & live[:, None]
    )
    return inside.astype(jnp.float32)


def mixing_weights(intersection):
    factor = jnp.linalg.cholesky(intersection)
    column = jnp.ones((intersection.shape[0], 1), intersection.dtype)
    middle = lax.linalg.triangular_solve(factor, column, left_side=True, lower=True)
    solved = lax.linalg.triangular_solve(
        factor, middle, left_side=True, lower=True, transpose_a=True
    )
    return solved[:, 0] / jnp.sum(solved)


def cosine_sine(length, freq_index, space_index):
    product = freq_index * space_index % length
    angle = 2.0 * math.pi / length * product.astype(jnp.float32)
    return (jnp.cos(angle), jnp.sin(angle))


def forward_spectra(fields, pencil_move, slab_move):
    batches, z_local, y_local, x_length = fields.shape
    pencil_count = lax.axis_size("pencil")
    slab_count = lax.axis_size("slab")
    x_columns = x_length // 2
    kx_local = x_columns // pencil_count
    y_length = y_local * pencil_count
    ky_local = y_length // slab_count
    z_length = z_local * slab_count
    freq_index = jnp.arange(x_columns, dtype=jnp.int32).reshape(pencil_count, kx_local, 1)
    space_index = jnp.arange(x_length, dtype=jnp.int32).reshape(1, 1, x_length)
    cosine, sine = cosine_sine(x_length, freq_index, space_index)
    nyquist = cosine_sine(x_length, jnp.full((1, 1, 1), x_length // 2, jnp.int32), space_index)[0]
    sine = jnp.where(freq_index == 0, -nyquist, sine)
    real_part = jnp.einsum("bzyx,pkx->bpkzy", fields, cosine, precision=highest)
    imag_part = -jnp.einsum("bzyx,pkx->bpkzy", fields, sine, precision=highest)
    packed = jnp.stack((real_part, imag_part), axis=1).reshape(batches, 2, pencil_count, -1)
    moved = pencil_move(packed).reshape(batches, 2, pencil_count, kx_local, z_local, y_local)
    freq_index = jnp.arange(y_length, dtype=jnp.int32).reshape(slab_count, ky_local, 1, 1)
    space_index = jnp.arange(y_length, dtype=jnp.int32).reshape(1, 1, pencil_count, y_local)
    cosine, sine = cosine_sine(y_length, freq_index, space_index)
    real_input = moved[:, 0]
    imag_input = moved[:, 1]
    form = "bskzy,glsy->bgklz"
    real_part = jnp.einsum(form, real_input, cosine, precision=highest) + jnp.einsum(
        form, imag_input, sine, precision=highest
    )
    imag_part = jnp.einsum(form, imag_input, cosine, precision=highest) - jnp.einsum(
        form, real_input, sine, precision=highest
    )
    packed = jnp.stack((real_part, imag_part), axis=1).reshape(batches, 2, slab_count, -1)
    moved = slab_move(packed).reshape(batches, 2, slab_count, kx_local, ky_local, z_local)
    freq_index = jnp.arange(z_length, dtype=jnp.int32).reshape(z_length, 1, 1)
    space_index = jnp.arange(z_length, dtype=jnp.int32).reshape(1, slab_count, z_local)
    cosine, sine = cosine_sine(z_length, freq_index, space_index)
    real_input = moved[:, 0]
    imag_input = moved[:, 1]
    form = "bgklz,mgz->bklm"
    real_part = jnp.einsum(form, real_input, cosine, precision=highest) + jnp.einsum(
        form, imag_input, sine, precision=highest
    )
    imag_part = jnp.einsum(form, imag_input, cosine, precision=highest) - jnp.einsum(
        form, real_input, sine, precision=highest
    )
    return jnp.stack((real_part, imag_part), axis=1)


def magnitude(index, length):
    return jnp.minimum(index, length - index).astype(jnp.float32)


def kerker_factor(freq_x, ky_local, x_length, y_length, z_length):
    freq_y = lax.axis_index("slab") * ky_local + jnp.arange(ky_local, dtype=jnp.int32)
    freq_z = jnp.arange(z_length, dtype=jnp.int32)
    square = (
        magnitude(freq_x, x_length)[:, None, None] ** 2
        + magnitude(freq_y, y_length)[None, :, None] ** 2
        + magnitude(freq_z, z_length)[None, None, :] ** 2
    )
    return square / (square + kerker_wave * kerker_wave)


def inverse_field(spectrum, z_local, y_local, x_length):
    pencil_count = lax.axis_size("pencil")
    slab_count = lax.axis_size("slab")
    x_columns = x_length // 2
    kx_local = x_columns // pencil_count
    slots = spectrum.shape[1]
    y_length = y_local * pencil_count
    ky_local = y_length // slab_count
    z_length = z_local * slab_count
    freq_index = jnp.arange(z_length, dtype=jnp.int32).reshape(z_length, 1, 1)
    space_index = jnp.arange(z_length, dtype=jnp.int32).reshape(1, slab_count, z_local)
    cosine, sine = cosine_sine(z_length, freq_index, space_index)
    real_input = spectrum[0]
    imag_input = spectrum[1]
    form = "klm,mdz->dklz"
    real_part = jnp.einsum(form, real_input, cosine, precision=highest) - jnp.einsum(
        form, imag_input, sine, precision=highest
    )
    imag_part = jnp.einsum(form, real_input, sine, precision=highest) + jnp.einsum(
        form, imag_input, cosine, precision=highest
    )
    packed = jnp.stack((real_part, imag_part), axis=0).reshape(2, slab_count, -1)
    moved = lax.all_to_all(packed, "slab", split_axis=1, concat_axis=1, tiled=True).reshape(
        2, slab_count, slots, ky_local, z_local
    )
    freq_index = jnp.arange(y_length, dtype=jnp.int32).reshape(slab_count, ky_local, 1, 1)
    space_index = jnp.arange(y_length, dtype=jnp.int32).reshape(1, 1, pencil_count, y_local)
    cosine, sine = cosine_sine(y_length, freq_index, space_index)
    real_input = moved[0]
    imag_input = moved[1]
    form = "gklz,glqy->qkzy"
    real_part = jnp.einsum(form, real_input, cosine, precision=highest) - jnp.einsum(
        form, imag_input, sine, precision=highest
    )
    imag_part = jnp.einsum(form, real_input, sine, precision=highest) + jnp.einsum(
        form, imag_input, cosine, precision=highest
    )
    packed = jnp.stack((real_part, imag_part), axis=0).reshape(2, pencil_count, -1)
    moved = lax.all_to_all(packed, "pencil", split_axis=1, concat_axis=1, tiled=True).reshape(
        2, pencil_count, slots, z_local, y_local
    )
    pencil_index = jnp.arange(pencil_count, dtype=jnp.int32).reshape(pencil_count, 1, 1)
    slot_index = jnp.arange(slots, dtype=jnp.int32).reshape(1, slots, 1)
    space_index = jnp.arange(x_length, dtype=jnp.int32).reshape(1, 1, x_length)
    freq_index = pencil_index * kx_local + slot_index
    cosine, sine = cosine_sine(x_length, freq_index, space_index)
    nyquist = cosine_sine(x_length, jnp.full((1, 1, 1), x_length // 2, jnp.int32), space_index)[0]
    ordinary = slot_index < kx_local
    doubling = jnp.where(freq_index == 0, 1.0, 2.0)
    real_table = jnp.where(ordinary, doubling * cosine, 0.0)
    imag_table = jnp.where(ordinary, -doubling * sine, jnp.where(pencil_index == 0, nyquist, 0.0))
    form = "pkzy,pkx->zyx"
    field = jnp.einsum(form, moved[0], real_table, precision=highest) + jnp.einsum(
        form, moved[1], imag_table, precision=highest
    )
    return field / (x_length * y_length * z_length)


def body(
    density_history, residual_history, occupancy_history, occupancy_residual, species, slot_count
):
    histories, z_local, y_local, x_length = residual_history.shape
    slab_count = lax.axis_size("slab")
    pencil_count = lax.axis_size("pencil")
    cell_total = z_local * slab_count * y_local * pencil_count * x_length
    slot_total = species.shape[0] * slab_count * pencil_count
    mask = block_mask(species, slot_count)
    flat = residual_history.reshape(histories, -1)
    grid_local = jnp.dot(flat, flat.T, precision=highest) / cell_total
    blocks = (occupancy_residual * mask[None]).reshape(histories, -1)
    block_local = jnp.dot(blocks, blocks.T, precision=highest) / (100.0 * slot_total)
    grid_intersection, block_intersection = lax.psum((grid_local, block_local), ("slab", "pencil"))
    weights = mixing_weights(grid_intersection + block_intersection)
    mixed = jnp.tensordot(weights, residual_history, axes=1, precision=highest)
    spectrum = forward_spectra(
        mixed[None],
        lambda packed: lax.all_to_all(packed, "pencil", split_axis=2, concat_axis=2, tiled=True),
        lambda packed: lax.all_to_all(packed, "slab", split_axis=2, concat_axis=2, tiled=True),
    )[0]
    x_columns = x_length // 2
    kx_local = x_columns // pencil_count
    y_length = y_local * pencil_count
    z_length = z_local * slab_count
    ky_local = y_length // slab_count
    freq_x = lax.axis_index("pencil") * kx_local + jnp.arange(kx_local, dtype=jnp.int32)
    factor = kerker_factor(freq_x, ky_local, x_length, y_length, z_length)
    filtered_spectrum = spectrum * factor[None]
    nyquist_x = jnp.full((1,), x_length // 2, jnp.int32)
    nyquist_factor = kerker_factor(nyquist_x, ky_local, x_length, y_length, z_length)
    owner = (lax.axis_index("pencil") == 0).astype(jnp.float32)
    extra = spectrum[:, 0:1] * nyquist_factor[None] * owner
    filtered_spectrum = jnp.concatenate((filtered_spectrum, extra), axis=1)
    filtered = inverse_field(filtered_spectrum, z_local, y_local, x_length)
    new_density = (
        jnp.tensordot(weights, density_history, axes=1, precision=highest) + grid_mixing * filtered
    )
    mixed_blocks = jnp.tensordot(
        weights, occupancy_history + block_mixing * occupancy_residual, axes=1, precision=highest
    )
    return (new_density, mask * mixed_blocks)


MESH = pl.DeviceIdType.MESH
VMEM_LIMIT = 40000 * 1024
GROUP = 1


def split(value):
    high = value.astype(jnp.bfloat16)
    low = (value - high.astype(jnp.float32)).astype(jnp.bfloat16)
    return high, low


def three(left, right, dims):
    numbers = (dims, ((), ()))
    dot = functools.partial(
        lax.dot_general, dimension_numbers=numbers, preferred_element_type=jnp.float32
    )
    return dot(left[1], right[0]) + dot(left[0], right[1]) + dot(left[0], right[0])


def halves(table):
    table = np.asarray(table, np.float32)
    high = table.astype(jnp.bfloat16)
    low = (table - high.astype(np.float32)).astype(jnp.bfloat16)
    return np.stack((high, low))


def waves(rows, columns, length):
    angle = 2.0 * np.pi / length * (np.outer(rows, columns) % length)
    return np.cos(angle), np.sin(angle)


def tables(x_length, y_length, z_length, pencil_count, slab_count):
    columns = x_length // 2
    cosine, sine = waves(np.arange(columns), np.arange(x_length), x_length)
    nyquist = np.where(np.arange(x_length) % 2 == 0, 1.0, -1.0)
    imag = -sine
    imag[0] = nyquist
    slots_k = columns // (pencil_count * slab_count)
    owner, slot = np.arange(columns) // slots_k, np.arange(columns) % slots_k
    chunk = np.searchsorted(cuts_of(slots_k), slot, side="right")
    order = np.lexsort((slot, owner, chunk))
    x_forward = np.stack((cosine, imag), axis=1)[order].reshape(x_length, x_length)
    doubling = np.where(np.arange(columns) == 0, 1.0, 2.0)[:, None]
    back = np.stack((doubling * cosine, doubling * imag), axis=1)[order]
    back = back.reshape(x_length, x_length)
    x_back = back * (grid_mixing / (x_length * y_length * z_length))
    cosine, sine = waves(np.arange(y_length), np.arange(y_length), y_length)
    along_y = np.stack((cosine, sine))
    cosine, sine = waves(np.arange(z_length), np.arange(z_length), z_length)
    order = np.arange(z_length).reshape(slab_count, -1).T.reshape(-1)
    cosine, sine = cosine[:, order], sine[:, order]
    z_forward = np.block([[cosine, sine], [-sine, cosine]])
    z_back = np.block([[cosine.T, -sine.T], [sine.T, cosine.T]])
    return [halves(t) for t in (x_forward, x_back, along_y, z_forward, z_back)]


def cuts_of(slots):
    return [at for at in range(1, slots, 2)] + [slots]


def pairs_of(count):
    return [(i, j) for i in range(count) for j in range(i + 1)]


def solve_weights(entry, count):
    lower, pivot = {}, []
    for j in range(count):
        scaled = [lower[j, k] * pivot[k] for k in range(j)]
        value = entry[j, j]
        for k in range(j):
            value = value - lower[j, k] * scaled[k]
        pivot.append(value)
        for i in range(j + 1, count):
            value = entry[i, j]
            for k in range(j):
                value = value - lower[i, k] * scaled[k]
            lower[i, j] = value / pivot[j]
    middle = []
    for i in range(count):
        value = jnp.ones_like(pivot[0])
        for k in range(i):
            value = value - lower[i, k] * middle[k]
        middle.append(value)
    solved = [None] * count
    for i in reversed(range(count)):
        value = middle[i] / pivot[i]
        for k in range(i + 1, count):
            value = value - lower[k, i] * solved[k]
        solved[i] = value
    total = solved[0]
    for value in solved[1:]:
        total = total + value
    return [value / total for value in solved]


def mix_kernel(
    slabs, pencils, cells, slots,
    live_ref, res_hbm, dens_hbm, occ_hbm, occ_res_hbm, species_hbm, corner_hbm,
    xf_hbm, yt_hbm, zf_hbm, zb_hbm, xb_hbm,
    out_ref, occ_out_ref, last,
    res, dens, occ_ref, occ_res_ref, species_ref, corner_ref,
    first_turn, sums, send_box, land_box, planes, spectrum, back_box, field,
    xf_ref, yt_ref, zf_ref, zb_ref, xb_ref,
    res_sem, table_sem, sum_sem, go_send, go_recv, back_send, back_recv,
):
    devices = slabs * pencils
    count, z_local, y_local, x_length = res.shape
    slots_k = x_length // 2 // devices
    freqs = 2 * slots_k
    z_length = z_local * slabs
    y_length = y_local * pencils
    tiles_out = send_box.shape[0]
    slab = lax.axis_index("slab")
    pencil = lax.axis_index("pencil")
    me = slab * pencils + pencil
    pairs = pairs_of(count)
    ends = cuts_of(slots_k)
    chunks = list(zip([0] + ends[:-1], ends))

    sources = (
        occ_res_hbm, species_hbm, corner_hbm, xf_hbm,
        occ_hbm, dens_hbm, yt_hbm, zf_hbm, zb_hbm, xb_hbm,
    )
    targets = (
        occ_res_ref, species_ref, corner_ref, xf_ref,
        occ_ref, dens, yt_ref, zf_ref, zb_ref, xb_ref,
    )
    loads = [
        pltpu.make_async_copy(a, b, table_sem.at[at])
        for at, (a, b) in enumerate(zip(sources, targets))
    ]

    def res_load(z):
        return pltpu.make_async_copy(res_hbm.at[:, z], res.at[:, z], res_sem.at[z])

    res_loads = [res_load(z) for z in range(z_local)]
    for copy in res_loads[:-1] + loads[:3] + res_loads[-1:] + loads[3:4]:
        copy.start()

    partners = []
    for step in range(1, devices):
        across = pencil + step % pencils
        row = lax.rem(slab + step // pencils + lax.div(across, pencils), slabs)
        column = lax.rem(across, pencils)
        partners.append(((row, column), row * pencils + column))

    barrier = pltpu.get_barrier_semaphore()

    for spot, _ in partners:
        pl.semaphore_signal(barrier, inc=1, device_id=spot, device_id_type=MESH)

    def wide(value):
        width = value.shape[1]
        if width == 128:
            return value
        return jnp.concatenate((value, jnp.zeros((8, 128 - width), value.dtype)), axis=1)

    def lanes_of(length):
        return [(at, min(at + 128, length)) for at in range(0, length, 128)]

    def plane(z, acc):
        acc = list(acc)
        res_load(z).wait()
        for row in range(0, y_local, 8):
            for start, stop in lanes_of(x_length):
                part = [wide(res[i, z, row:row + 8, start:stop]) for i in range(count)]
                for at, (i, j) in enumerate(pairs):
                    acc[at] = acc[at] + part[i] * part[j]
        return tuple(acc)

    nothing = tuple(jnp.zeros((8, 128), jnp.float32) for _ in pairs)
    acc = lax.fori_loop(0, z_local - 1, plane, nothing)
    for copy in loads[:3]:
        copy.wait()
    slot_count, entries = occ_ref.shape[1:]
    species = species_ref[...]
    orbitals = jnp.zeros_like(species)
    for species_index, orbital_number in enumerate(species_orbitals):
        orbitals = jnp.where(species == species_index, orbital_number, orbitals)
    square = (slot_count, slot_count)
    row_index = lax.broadcasted_iota(jnp.int32, square, 0)
    column_index = lax.broadcasted_iota(jnp.int32, square, 1)
    chosen = (row_index == column_index) & (column_index < live_ref[0])
    limit = jnp.sum(
        jnp.where(chosen, orbitals.astype(jnp.float32), 0.0), axis=1, keepdims=True
    )
    mask = (corner_ref[...] < limit).astype(jnp.float32)
    ratio = cells / (100.0 * slots)
    blocks_acc = [jnp.zeros((8, 128), jnp.float32) for _ in pairs]
    for first in range(0, slot_count, 8):
        for start, stop in lanes_of(entries):
            part = [
                wide(occ_res_ref[i, first:first + 8, start:stop] * mask[first:first + 8, start:stop])
                for i in range(count)
            ]
            for at, (i, j) in enumerate(pairs):
                blocks_acc[at] = blocks_acc[at] + part[i] * part[j]
    acc = [value + blocks * ratio for value, blocks in zip(acc, blocks_acc)]
    acc = plane(z_local - 1, acc)

    for copy in loads[4:]:
        copy.start()
    stacked = jnp.concatenate([jnp.sum(a, axis=0, keepdims=True) for a in acc], axis=0)
    totals = jnp.sum(stacked, axis=1, keepdims=True) / cells
    shape = (len(pairs), 128)
    pair_index = lax.broadcasted_iota(jnp.int32, shape, 0)
    across = lax.broadcasted_iota(jnp.int32, shape, 1)
    packed = jnp.sum(jnp.where(pair_index == across, totals, 0.0), axis=0, keepdims=True)
    sums[pl.ds(me, 1), :] = packed

    pl.semaphore_wait(barrier, devices - 1)

    for spot, _ in partners:
        pltpu.make_async_remote_copy(
            src_ref=sums.at[pl.ds(me, 1)], dst_ref=sums.at[pl.ds(me, 1)],
            send_sem=sum_sem.at[0], recv_sem=sum_sem.at[1],
            device_id=spot, device_id_type=MESH,
        ).start()
    all_sums = pltpu.make_async_remote_copy(
        src_ref=sums.at[pl.ds(0, devices - 1)], dst_ref=sums.at[pl.ds(0, devices - 1)],
        send_sem=sum_sem.at[0], recv_sem=sum_sem.at[1],
        device_id=partners[0][0], device_id_type=MESH,
    )

    loads[3].wait()
    opening = slice(0, 2 * ends[0] * devices)

    left = (xf_ref[0, opening, :], xf_ref[1, opening, :])
    for i in range(count):
        history = split(res[i].reshape(z_local * y_local, x_length))
        first_turn[i] = three(left, history, ((1,), (1,)))

    all_sums.wait_recv()
    gathered = jnp.sum(sums[...], axis=0, keepdims=True)
    lane_index = lax.broadcasted_iota(jnp.int32, (1, 128), 1)
    entry = {
        pair: jnp.sum(jnp.where(lane_index == at, gathered, 0.0), axis=1, keepdims=True)
        for at, pair in enumerate(pairs)
    }
    weights = solve_weights(entry, count)

    def share(chunk, index):
        first, end = chunks[chunk]
        size = 2 * (end - first)
        return pl.ds(2 * first * devices + index * size, size)

    def go_copy(chunk, spot, target):
        return pltpu.make_async_remote_copy(
            src_ref=send_box.at[:, share(chunk, target), :],
            dst_ref=land_box.at[:, share(chunk, me), :],
            send_sem=go_send.at[0], recv_sem=go_recv.at[chunk],
            device_id=spot, device_id_type=MESH,
        )

    def landing(chunk, rows):
        if chunk < len(chunks) - 1:
            return field.at[:, rows, :]
        return last.at[:, pl.ds(rows.start - 2 * chunks[chunk][0] * devices, rows.size), :]

    def back_copy(chunk, spot, target):
        return pltpu.make_async_remote_copy(
            src_ref=back_box.at[:, share(chunk, target), :],
            dst_ref=landing(chunk, share(chunk, me)),
            send_sem=back_send.at[0], recv_sem=back_recv.at[chunk],
            device_id=spot, device_id_type=MESH,
        )

    def start_all(copy, chunk):
        for spot, target in partners:
            copy(chunk, spot, target).start()

    def whole(source, target, rows, send, recv):
        return pltpu.make_async_remote_copy(
            src_ref=source.at[:, rows, :], dst_ref=target.at[:, rows, :],
            send_sem=send, recv_sem=recv, device_id=partners[0][0], device_id_type=MESH,
        )

    def land_all(source, target, send, recv, chunk):
        first, end = chunks[chunk]
        rows = pl.ds(2 * first * devices, 2 * (end - first) * (devices - 1))
        whole(source, target, rows, send.at[0], recv.at[chunk]).wait_recv()

    def drain_all(source, target, send, recv):
        rows = pl.ds(0, freqs * (devices - 1))
        whole(source, target, rows, send.at[0], recv.at[0]).wait_send()

    def mixed(parts):
        total = weights[0] * parts[0]
        for i in range(1, count):
            total = total + weights[i] * parts[i]
        return total

    turned = mixed([first_turn[i] for i in range(count)])
    for t in range(tiles_out):
        send_box[t, opening, :] = turned[:, t * 128:(t + 1) * 128]
    start_all(go_copy, 0)
    land_box[:, share(0, me), :] = send_box[:, share(0, me), :]

    mixture = [mixed([res[i, z] for i in range(count)]) for z in range(z_local)]
    mixture = split(jnp.concatenate(mixture, axis=0))
    for chunk, (first, end) in enumerate(chunks):
        if chunk == 0:
            continue
        rows = slice(2 * first * devices, 2 * end * devices)
        turned = three((xf_ref[0, rows, :], xf_ref[1, rows, :]), mixture, ((1,), (1,)))
        for t in range(tiles_out):
            send_box[t, rows, :] = turned[:, t * 128:(t + 1) * 128]
        start_all(go_copy, chunk)
        land_box[:, share(chunk, me), :] = send_box[:, share(chunk, me), :]

    for copy in loads[4:]:
        copy.wait()
    for z in range(z_local):
        out_ref[z * y_local:(z + 1) * y_local, :] = mixed([dens[i, z] for i in range(count)])
    occ_out_ref[...] = mask * mixed(
        [occ_ref[i] + block_mixing * occ_res_ref[i] for i in range(count)]
    )
    all_sums.wait_send()

    z_forward = (zf_ref[0], zf_ref[1])
    z_back = (zb_ref[0], zb_ref[1])
    y_cosine = (yt_ref[0, 0], yt_ref[1, 0])
    y_sine = (yt_ref[0, 1], yt_ref[1, 1])
    shape = (2 * z_length, y_length)
    z_index = lax.rem(lax.broadcasted_iota(jnp.int32, shape, 0), z_length)
    y_index = lax.broadcasted_iota(jnp.int32, shape, 1)
    z_size = jnp.minimum(z_index, z_length - z_index).astype(jnp.float32)
    y_size = jnp.minimum(y_index, y_length - y_index).astype(jnp.float32)
    flat = z_size * z_size + y_size * y_size

    def filtered(wave, freq_x):
        size = freq_x.astype(jnp.float32)
        square = flat + size * size
        return split(wave * (square / (square + kerker_wave * kerker_wave)))

    for chunk, (first, end) in enumerate(chunks):
        size = 2 * (end - first)
        base = 2 * first * devices
        land_all(send_box, land_box, go_send, go_recv, chunk)
        for p in range(pencils):
            for f in range(size):
                joined = jnp.concatenate(
                    [
                        land_box[t, pl.ds(base + p * size + f, slabs, stride=pencils * size), :]
                        for t in range(tiles_out)
                    ],
                    axis=1,
                )
                for z in range(z_local):
                    planes[
                        2 * first + f, z * slabs:(z + 1) * slabs, p * y_local:(p + 1) * y_local
                    ] = joined[:, z * y_local:(z + 1) * y_local]
        block = split(planes[2 * first:2 * end].reshape(size * z_length, y_length))
        along_cosine = three(block, y_cosine, ((1,), (0,)))
        along_sine = three(block, y_sine, ((1,), (0,)))
        extra = first == 0
        for k in range(first, end):
            top, low = 2 * (k - first) * z_length, (2 * (k - first) + 1) * z_length
            stop = low + z_length
            real = along_cosine[top:low] + along_sine[low:stop]
            imag = along_cosine[low:stop] - along_sine[top:low]
            wave = three(z_forward, split(jnp.concatenate((real, imag), axis=0)), ((1,), (0,)))
            freq_x = me * slots_k + k
            spectrum[k - first] = three(z_back, filtered(wave, freq_x), ((1,), (0,)))
            if k == 0:
                freq_x = jnp.where(me == 0, x_length // 2, freq_x)
                spectrum[end] = three(z_back, filtered(wave, freq_x), ((1,), (0,)))
        used = end - first + (1 if extra else 0)
        block = split(spectrum[0:used].reshape(used * 2 * z_length, y_length))
        along_cosine = three(block, y_cosine, ((1,), (0,)))
        along_sine = three(block, y_sine, ((1,), (0,)))
        for k in range(first, end):
            top, low = 2 * (k - first) * z_length, (2 * (k - first) + 1) * z_length
            stop = low + z_length
            real = along_cosine[top:low] - along_sine[low:stop]
            if k == 0:
                top, low = 2 * end * z_length, (2 * end + 1) * z_length
                stop = low + z_length
            imag = along_cosine[low:stop] + along_sine[top:low]
            for c, part in enumerate((real, imag)):
                for p in range(pencils):
                    joined = jnp.concatenate(
                        [
                            part[z * slabs:(z + 1) * slabs, p * y_local:(p + 1) * y_local]
                            for z in range(z_local)
                        ],
                        axis=1,
                    )
                    start = base + p * size + 2 * (k - first) + c
                    for t in range(tiles_out):
                        back_box[t, pl.ds(start, slabs, stride=pencils * size), :] = joined[
                            :, t * 128:(t + 1) * 128
                        ]
        start_all(back_copy, chunk)
        landing(chunk, share(chunk, me))[...] = back_box[:, share(chunk, me), :]

    drain_all(send_box, land_box, go_send, go_recv)
    for chunk, (first, end) in enumerate(chunks):
        rows = pl.ds(2 * first * devices, 2 * (end - first) * (devices - 1))
        pltpu.make_async_remote_copy(
            src_ref=back_box.at[:, rows, :], dst_ref=landing(chunk, rows),
            send_sem=back_send.at[0], recv_sem=back_recv.at[chunk],
            device_id=partners[0][0], device_id_type=MESH,
        ).wait_recv()
        if chunk == len(chunks) - 1:
            continue
        used = slice(2 * first * devices, 2 * end * devices)
        table = (xb_ref[0, used, :], xb_ref[1, used, :])
        for t in range(tiles_out):
            rows = slice(t * 128, (t + 1) * 128)
            out_ref[rows, :] = out_ref[rows, :] + three(
                split(field[t, used, :]), table, ((0,), (0,))
            )
    drain_all(back_box, back_box, back_send, back_recv)


def finish_kernel(last, dens_ref, occ_ref, xb_ref, out_hbm, occ_hbm, out_ref, sem):
    tiles, depth, _ = last.shape
    copies = [pltpu.make_async_copy(occ_ref, occ_hbm, sem.at[tiles])]
    copies[0].start()
    dot = functools.partial(
        lax.dot_general,
        dimension_numbers=(((0,), (0,)), ((), ())),
        preferred_element_type=jnp.float32,
    )
    for first in range(0, tiles, GROUP):
        end = min(first + GROUP, tiles)
        high, low = split(jnp.concatenate([last[t] for t in range(first, end)], axis=1))
        both = jnp.concatenate((high, low), axis=0)
        turned = dot(both, xb_ref[:2 * depth]) + dot(high, xb_ref[2 * depth:])
        rows = slice(first * 128, end * 128)
        out_ref[rows, :] = dens_ref[rows, :] + turned
        copies.append(pltpu.make_async_copy(out_ref.at[rows], out_hbm.at[rows], sem.at[first]))
        copies[-1].start()
    for copy in copies:
        copy.wait()


def fused_body(
    density_history, residual_history, occupancy_history, occupancy_residual, species, slot_count
):
    count, z_local, y_local, x_length = residual_history.shape
    slabs = lax.axis_size("slab")
    pencils = lax.axis_size("pencil")
    devices = slabs * pencils
    z_length, y_length = z_local * slabs, y_local * pencils
    freqs = x_length // devices
    entry = np.arange(ORBITALS * ORBITALS)
    corner = np.maximum(entry // ORBITALS, entry % ORBITALS)[None].astype(np.float32)
    x_forward, x_back, *others = tables(x_length, y_length, z_length, pencils, slabs)
    constants = [x_forward, *others, x_back]
    ends = cuts_of(freqs // 2)
    chunks = len(ends)
    late = 2 * ends[-2] * devices if chunks > 1 else 0
    constants[-1] = x_back[:, :late] if late else x_back[:, :16]
    constants = [jnp.asarray(t) for t in constants]
    vmem = pl.BlockSpec(memory_space=pltpu.VMEM)
    hbm = pl.BlockSpec(memory_space=pltpu.HBM)
    box = (z_local * y_local // 128, devices * freqs, 128)
    sems = pltpu.SemaphoreType.DMA
    flat = jax.ShapeDtypeStruct((z_local * y_local, x_length), jnp.float32)
    blocks = jax.ShapeDtypeStruct(occupancy_history.shape[1:], jnp.float32)
    smalls = [
        occupancy_history, occupancy_residual, species[None], jnp.asarray(corner)
    ]
    mixed, mixed_blocks, last = pl.pallas_call(
        functools.partial(
            mix_kernel, slabs, pencils,
            z_length * y_length * x_length, species.shape[0] * devices,
        ),
        out_shape=(flat, blocks, jax.ShapeDtypeStruct((box[0], box[1] - late, 128), jnp.float32)),
        in_specs=[pl.BlockSpec(memory_space=pltpu.SMEM)] + [hbm] * (6 + len(constants)),
        out_specs=(vmem, vmem, vmem),
        scratch_shapes=[
            pltpu.VMEM(residual_history.shape, jnp.float32),
            pltpu.VMEM(residual_history.shape, jnp.float32),
            *[pltpu.VMEM(t.shape, t.dtype) for t in smalls],
            pltpu.VMEM((count, 2 * ends[0] * devices, z_local * y_local), jnp.float32),
            pltpu.VMEM((devices, 128), jnp.float32),
            pltpu.VMEM(box, jnp.float32),
            pltpu.VMEM(box, jnp.float32),
            pltpu.VMEM((freqs, z_length, y_length), jnp.float32),
            pltpu.VMEM((freqs // 2 + 1, 2 * z_length, y_length), jnp.float32),
            pltpu.VMEM(box, jnp.float32),
            pltpu.VMEM((box[0], late or 16, 128), jnp.float32),
            *[pltpu.VMEM(t.shape, t.dtype) for t in constants],
            sems((z_local,)),
            sems((5 + len(constants),)),
            sems((2,)),
            sems((1,)), sems((chunks,)),
            sems((1,)), sems((chunks,)),
        ],
        compiler_params=pltpu.CompilerParams(
            collective_id=0, has_side_effects=True, vmem_limit_bytes=VMEM_LIMIT
        ),
    )(slot_count, *[
        pltpu.with_memory_space_constraint(value, pltpu.HBM)
        for value in (residual_history, density_history, *smalls, *constants)
    ])
    tiles = box[0]
    new_density, new_blocks = pl.pallas_call(
        finish_kernel,
        out_shape=(flat, blocks),
        in_specs=[vmem] * 4,
        out_specs=(hbm, hbm),
        scratch_shapes=[pltpu.VMEM(flat.shape, flat.dtype), sems((tiles + 1,))],
        compiler_params=pltpu.CompilerParams(vmem_limit_bytes=8 * 1024 * 1024),
    )(last, mixed, mixed_blocks, jnp.asarray(np.concatenate((x_back[0, late:], *x_back[:, late:]))))
    return new_density.reshape(z_local, y_local, x_length), new_blocks


def solution(mesh):
    placed = (
        P(None, "slab", "pencil", None),
        P(None, "slab", "pencil", None),
        P(None, ("slab", "pencil"), None),
        P(None, ("slab", "pencil"), None),
        P(("slab", "pencil")),
        P(("slab", "pencil")),
    )
    devices = mesh.shape["slab"] * mesh.shape["pencil"]

    def chosen(*arrays):
        x_length = arrays[0].shape[3]
        _, z_local, y_local, _ = arrays[0].shape
        fits = (
            x_length % (2 * devices) == 0
            and mesh.shape["slab"] % 8 == 0
            and y_local % 16 == 0
            and z_local * y_local % 128 == 0
        )
        return (fused_body if fits else body)(*arrays)

    return jax.shard_map(
        chosen,
        mesh=mesh,
        in_specs=placed,
        out_specs=(P("slab", "pencil", None), P(("slab", "pencil"), None)),
        check_vma=False,
    )
```

```python
import functools
import math

import jax
import jax.numpy as jnp
import numpy as np
from jax import lax
from jax.experimental import pallas as pl
from jax.experimental.pallas import tpu as pltpu
from jax.sharding import PartitionSpec as P

ORBITALS = 18


highest = lax.Precision.HIGHEST
grid_mixing = 0.5
block_mixing = 0.5
kerker_wave = 6.0
species_orbitals = (18, 13, 8, 5)


def block_mask(species, slot_count):
    live = jnp.arange(species.shape[0], dtype=jnp.int32) < slot_count[0]
    orbitals = jnp.zeros_like(species)
    for species_index, orbital_number in enumerate(species_orbitals):
        orbitals = orbitals + orbital_number * (species == species_index).astype(jnp.int32)
    entry = jnp.arange(ORBITALS * ORBITALS, dtype=jnp.int32)
    row_index = entry // ORBITALS
    column_index = entry % ORBITALS
    inside = (
        (row_index[None, :] < orbitals[:, None])
        & (column_index[None, :] < orbitals[:, None])
        & live[:, None]
    )
    return inside.astype(jnp.float32)


def mixing_weights(intersection):
    factor = jnp.linalg.cholesky(intersection)
    column = jnp.ones((intersection.shape[0], 1), intersection.dtype)
    middle = lax.linalg.triangular_solve(factor, column, left_side=True, lower=True)
    solved = lax.linalg.triangular_solve(
        factor, middle, left_side=True, lower=True, transpose_a=True
    )
    return solved[:, 0] / jnp.sum(solved)


def cosine_sine(length, freq_index, space_index):
    product = freq_index * space_index % length
    angle = 2.0 * math.pi / length * product.astype(jnp.float32)
    return (jnp.cos(angle), jnp.sin(angle))


def forward_spectra(fields, pencil_move, slab_move):
    batches, z_local, y_local, x_length = fields.shape
    pencil_count = lax.axis_size("pencil")
    slab_count = lax.axis_size("slab")
    x_columns = x_length // 2
    kx_local = x_columns // pencil_count
    y_length = y_local * pencil_count
    ky_local = y_length // slab_count
    z_length = z_local * slab_count
    freq_index = jnp.arange(x_columns, dtype=jnp.int32).reshape(pencil_count, kx_local, 1)
    space_index = jnp.arange(x_length, dtype=jnp.int32).reshape(1, 1, x_length)
    cosine, sine = cosine_sine(x_length, freq_index, space_index)
    nyquist = cosine_sine(x_length, jnp.full((1, 1, 1), x_length // 2, jnp.int32), space_index)[0]
    sine = jnp.where(freq_index == 0, -nyquist, sine)
    real_part = jnp.einsum("bzyx,pkx->bpkzy", fields, cosine, precision=highest)
    imag_part = -jnp.einsum("bzyx,pkx->bpkzy", fields, sine, precision=highest)
    packed = jnp.stack((real_part, imag_part), axis=1).reshape(batches, 2, pencil_count, -1)
    moved = pencil_move(packed).reshape(batches, 2, pencil_count, kx_local, z_local, y_local)
    freq_index = jnp.arange(y_length, dtype=jnp.int32).reshape(slab_count, ky_local, 1, 1)
    space_index = jnp.arange(y_length, dtype=jnp.int32).reshape(1, 1, pencil_count, y_local)
    cosine, sine = cosine_sine(y_length, freq_index, space_index)
    real_input = moved[:, 0]
    imag_input = moved[:, 1]
    form = "bskzy,glsy->bgklz"
    real_part = jnp.einsum(form, real_input, cosine, precision=highest) + jnp.einsum(
        form, imag_input, sine, precision=highest
    )
    imag_part = jnp.einsum(form, imag_input, cosine, precision=highest) - jnp.einsum(
        form, real_input, sine, precision=highest
    )
    packed = jnp.stack((real_part, imag_part), axis=1).reshape(batches, 2, slab_count, -1)
    moved = slab_move(packed).reshape(batches, 2, slab_count, kx_local, ky_local, z_local)
    freq_index = jnp.arange(z_length, dtype=jnp.int32).reshape(z_length, 1, 1)
    space_index = jnp.arange(z_length, dtype=jnp.int32).reshape(1, slab_count, z_local)
    cosine, sine = cosine_sine(z_length, freq_index, space_index)
    real_input = moved[:, 0]
    imag_input = moved[:, 1]
    form = "bgklz,mgz->bklm"
    real_part = jnp.einsum(form, real_input, cosine, precision=highest) + jnp.einsum(
        form, imag_input, sine, precision=highest
    )
    imag_part = jnp.einsum(form, imag_input, cosine, precision=highest) - jnp.einsum(
        form, real_input, sine, precision=highest
    )
    return jnp.stack((real_part, imag_part), axis=1)


def magnitude(index, length):
    return jnp.minimum(index, length - index).astype(jnp.float32)


def kerker_factor(freq_x, ky_local, x_length, y_length, z_length):
    freq_y = lax.axis_index("slab") * ky_local + jnp.arange(ky_local, dtype=jnp.int32)
    freq_z = jnp.arange(z_length, dtype=jnp.int32)
    square = (
        magnitude(freq_x, x_length)[:, None, None] ** 2
        + magnitude(freq_y, y_length)[None, :, None] ** 2
        + magnitude(freq_z, z_length)[None, None, :] ** 2
    )
    return square / (square + kerker_wave * kerker_wave)


def inverse_field(spectrum, z_local, y_local, x_length):
    pencil_count = lax.axis_size("pencil")
    slab_count = lax.axis_size("slab")
    x_columns = x_length // 2
    kx_local = x_columns // pencil_count
    slots = spectrum.shape[1]
    y_length = y_local * pencil_count
    ky_local = y_length // slab_count
    z_length = z_local * slab_count
    freq_index = jnp.arange(z_length, dtype=jnp.int32).reshape(z_length, 1, 1)
    space_index = jnp.arange(z_length, dtype=jnp.int32).reshape(1, slab_count, z_local)
    cosine, sine = cosine_sine(z_length, freq_index, space_index)
    real_input = spectrum[0]
    imag_input = spectrum[1]
    form = "klm,mdz->dklz"
    real_part = jnp.einsum(form, real_input, cosine, precision=highest) - jnp.einsum(
        form, imag_input, sine, precision=highest
    )
    imag_part = jnp.einsum(form, real_input, sine, precision=highest) + jnp.einsum(
        form, imag_input, cosine, precision=highest
    )
    packed = jnp.stack((real_part, imag_part), axis=0).reshape(2, slab_count, -1)
    moved = lax.all_to_all(packed, "slab", split_axis=1, concat_axis=1, tiled=True).reshape(
        2, slab_count, slots, ky_local, z_local
    )
    freq_index = jnp.arange(y_length, dtype=jnp.int32).reshape(slab_count, ky_local, 1, 1)
    space_index = jnp.arange(y_length, dtype=jnp.int32).reshape(1, 1, pencil_count, y_local)
    cosine, sine = cosine_sine(y_length, freq_index, space_index)
    real_input = moved[0]
    imag_input = moved[1]
    form = "gklz,glqy->qkzy"
    real_part = jnp.einsum(form, real_input, cosine, precision=highest) - jnp.einsum(
        form, imag_input, sine, precision=highest
    )
    imag_part = jnp.einsum(form, real_input, sine, precision=highest) + jnp.einsum(
        form, imag_input, cosine, precision=highest
    )
    packed = jnp.stack((real_part, imag_part), axis=0).reshape(2, pencil_count, -1)
    moved = lax.all_to_all(packed, "pencil", split_axis=1, concat_axis=1, tiled=True).reshape(
        2, pencil_count, slots, z_local, y_local
    )
    pencil_index = jnp.arange(pencil_count, dtype=jnp.int32).reshape(pencil_count, 1, 1)
    slot_index = jnp.arange(slots, dtype=jnp.int32).reshape(1, slots, 1)
    space_index = jnp.arange(x_length, dtype=jnp.int32).reshape(1, 1, x_length)
    freq_index = pencil_index * kx_local + slot_index
    cosine, sine = cosine_sine(x_length, freq_index, space_index)
    nyquist = cosine_sine(x_length, jnp.full((1, 1, 1), x_length // 2, jnp.int32), space_index)[0]
    ordinary = slot_index < kx_local
    doubling = jnp.where(freq_index == 0, 1.0, 2.0)
    real_table = jnp.where(ordinary, doubling * cosine, 0.0)
    imag_table = jnp.where(ordinary, -doubling * sine, jnp.where(pencil_index == 0, nyquist, 0.0))
    form = "pkzy,pkx->zyx"
    field = jnp.einsum(form, moved[0], real_table, precision=highest) + jnp.einsum(
        form, moved[1], imag_table, precision=highest
    )
    return field / (x_length * y_length * z_length)


def body(
    density_history, residual_history, occupancy_history, occupancy_residual, species, slot_count
):
    histories, z_local, y_local, x_length = residual_history.shape
    slab_count = lax.axis_size("slab")
    pencil_count = lax.axis_size("pencil")
    cell_total = z_local * slab_count * y_local * pencil_count * x_length
    slot_total = species.shape[0] * slab_count * pencil_count
    mask = block_mask(species, slot_count)
    flat = residual_history.reshape(histories, -1)
    grid_local = jnp.dot(flat, flat.T, precision=highest) / cell_total
    blocks = (occupancy_residual * mask[None]).reshape(histories, -1)
    block_local = jnp.dot(blocks, blocks.T, precision=highest) / (100.0 * slot_total)
    grid_intersection, block_intersection = lax.psum((grid_local, block_local), ("slab", "pencil"))
    weights = mixing_weights(grid_intersection + block_intersection)
    mixed = jnp.tensordot(weights, residual_history, axes=1, precision=highest)
    spectrum = forward_spectra(
        mixed[None],
        lambda packed: lax.all_to_all(packed, "pencil", split_axis=2, concat_axis=2, tiled=True),
        lambda packed: lax.all_to_all(packed, "slab", split_axis=2, concat_axis=2, tiled=True),
    )[0]
    x_columns = x_length // 2
    kx_local = x_columns // pencil_count
    y_length = y_local * pencil_count
    z_length = z_local * slab_count
    ky_local = y_length // slab_count
    freq_x = lax.axis_index("pencil") * kx_local + jnp.arange(kx_local, dtype=jnp.int32)
    factor = kerker_factor(freq_x, ky_local, x_length, y_length, z_length)
    filtered_spectrum = spectrum * factor[None]
    nyquist_x = jnp.full((1,), x_length // 2, jnp.int32)
    nyquist_factor = kerker_factor(nyquist_x, ky_local, x_length, y_length, z_length)
    owner = (lax.axis_index("pencil") == 0).astype(jnp.float32)
    extra = spectrum[:, 0:1] * nyquist_factor[None] * owner
    filtered_spectrum = jnp.concatenate((filtered_spectrum, extra), axis=1)
    filtered = inverse_field(filtered_spectrum, z_local, y_local, x_length)
    new_density = (
        jnp.tensordot(weights, density_history, axes=1, precision=highest) + grid_mixing * filtered
    )
    mixed_blocks = jnp.tensordot(
        weights, occupancy_history + block_mixing * occupancy_residual, axes=1, precision=highest
    )
    return (new_density, mask * mixed_blocks)


MESH = pl.DeviceIdType.MESH
VMEM_LIMIT = 40000 * 1024
GROUP = 1


def split(value):
    high = value.astype(jnp.bfloat16)
    low = (value - high.astype(jnp.float32)).astype(jnp.bfloat16)
    return high, low


def three(left, right, dims):
    numbers = (dims, ((), ()))
    dot = functools.partial(
        lax.dot_general, dimension_numbers=numbers, preferred_element_type=jnp.float32
    )
    return dot(left[1], right[0]) + dot(left[0], right[1]) + dot(left[0], right[0])


def halves(table):
    table = np.asarray(table, np.float32)
    high = table.astype(jnp.bfloat16)
    low = (table - high.astype(np.float32)).astype(jnp.bfloat16)
    return np.stack((high, low))


def waves(rows, columns, length):
    angle = 2.0 * np.pi / length * (np.outer(rows, columns) % length)
    return np.cos(angle), np.sin(angle)


def tables(x_length, y_length, z_length, pencil_count, slab_count):
    columns = x_length // 2
    cosine, sine = waves(np.arange(columns), np.arange(x_length), x_length)
    nyquist = np.where(np.arange(x_length) % 2 == 0, 1.0, -1.0)
    imag = -sine
    imag[0] = nyquist
    slots_k = columns // (pencil_count * slab_count)
    owner, slot = np.arange(columns) // slots_k, np.arange(columns) % slots_k
    chunk = np.searchsorted(cuts_of(slots_k), slot, side="right")
    order = np.lexsort((slot, owner, chunk))
    x_forward = np.stack((cosine, imag), axis=1)[order].reshape(x_length, x_length)
    doubling = np.where(np.arange(columns) == 0, 1.0, 2.0)[:, None]
    back = np.stack((doubling * cosine, doubling * imag), axis=1)[order]
    back = back.reshape(x_length, x_length)
    x_back = back * (grid_mixing / (x_length * y_length * z_length))
    cosine, sine = waves(np.arange(y_length), np.arange(y_length), y_length)
    along_y = np.stack((cosine, sine))
    cosine, sine = waves(np.arange(z_length), np.arange(z_length), z_length)
    order = np.arange(z_length).reshape(slab_count, -1).T.reshape(-1)
    cosine, sine = cosine[:, order], sine[:, order]
    z_forward = np.block([[cosine, sine], [-sine, cosine]])
    z_back = np.block([[cosine.T, -sine.T], [sine.T, cosine.T]])
    return [halves(t) for t in (x_forward, x_back, along_y, z_forward, z_back)]


def cuts_of(slots):
    return [at for at in range(1, slots, 2)] + [slots]


def pairs_of(count):
    return [(i, j) for i in range(count) for j in range(i + 1)]


def solve_weights(entry, count):
    lower, pivot = {}, []
    for j in range(count):
        scaled = [lower[j, k] * pivot[k] for k in range(j)]
        value = entry[j, j]
        for k in range(j):
            value = value - lower[j, k] * scaled[k]
        pivot.append(value)
        for i in range(j + 1, count):
            value = entry[i, j]
            for k in range(j):
                value = value - lower[i, k] * scaled[k]
            lower[i, j] = value / pivot[j]
    middle = []
    for i in range(count):
        value = jnp.ones_like(pivot[0])
        for k in range(i):
            value = value - lower[i, k] * middle[k]
        middle.append(value)
    solved = [None] * count
    for i in reversed(range(count)):
        value = middle[i] / pivot[i]
        for k in range(i + 1, count):
            value = value - lower[k, i] * solved[k]
        solved[i] = value
    total = solved[0]
    for value in solved[1:]:
        total = total + value
    return [value / total for value in solved]


def mix_kernel(
    slabs, pencils, cells, slots,
    live_ref, res_hbm, dens_hbm, occ_hbm, occ_res_hbm, species_hbm, corner_hbm,
    xf_hbm, yt_hbm, zf_hbm, zb_hbm, xb_hbm,
    out_ref, occ_out_ref, last,
    res, dens, occ_ref, occ_res_ref, species_ref, corner_ref,
    first_turn, sums, send_box, land_box, planes, spectrum, back_box, field,
    xf_ref, yt_ref, zf_ref, zb_ref, xb_ref,
    res_sem, table_sem, sum_sem, go_send, go_recv, back_send, back_recv,
):
    devices = slabs * pencils
    count, z_local, y_local, x_length = res.shape
    slots_k = x_length // 2 // devices
    freqs = 2 * slots_k
    z_length = z_local * slabs
    y_length = y_local * pencils
    tiles_out = send_box.shape[0]
    slab = lax.axis_index("slab")
    pencil = lax.axis_index("pencil")
    me = slab * pencils + pencil
    pairs = pairs_of(count)
    ends = cuts_of(slots_k)
    chunks = list(zip([0] + ends[:-1], ends))

    sources = (
        occ_res_hbm, species_hbm, corner_hbm, xf_hbm,
        occ_hbm, dens_hbm, yt_hbm, zf_hbm, zb_hbm, xb_hbm,
    )
    targets = (
        occ_res_ref, species_ref, corner_ref, xf_ref,
        occ_ref, dens, yt_ref, zf_ref, zb_ref, xb_ref,
    )
    loads = [
        pltpu.make_async_copy(a, b, table_sem.at[at])
        for at, (a, b) in enumerate(zip(sources, targets))
    ]

    half = y_local // 16 * 8
    end_plane = z_local - 1

    def res_load(z, first, size, at):
        rows = pl.ds(first, size)
        return pltpu.make_async_copy(
            res_hbm.at[:, z, rows], res.at[:, z, rows], res_sem.at[at]
        )

    open_loads = [
        res_load(0, 0, half, 0), res_load(0, half, y_local - half, z_local)
    ]
    res_loads = [res_load(z, 0, y_local, z) for z in range(1, end_plane)]
    end_loads = [
        res_load(end_plane, 0, half, end_plane),
        res_load(end_plane, half, y_local - half, z_local + 1),
    ]
    for copy in open_loads + res_loads + loads[:3] + end_loads + loads[3:4]:
        copy.start()

    partners = []
    for step in range(1, devices):
        across = pencil + step % pencils
        row = lax.rem(slab + step // pencils + lax.div(across, pencils), slabs)
        column = lax.rem(across, pencils)
        partners.append(((row, column), row * pencils + column))

    barrier = pltpu.get_barrier_semaphore()

    for spot, _ in partners:
        pl.semaphore_signal(barrier, inc=1, device_id=spot, device_id_type=MESH)

    def wide(value):
        width = value.shape[1]
        if width == 128:
            return value
        return jnp.concatenate((value, jnp.zeros((8, 128 - width), value.dtype)), axis=1)

    def lanes_of(length):
        return [(at, min(at + 128, length)) for at in range(0, length, 128)]

    def add_rows(z, first, end, acc):
        acc = list(acc)
        for row in range(first, end, 8):
            for start, stop in lanes_of(x_length):
                part = [wide(res[i, z, row:row + 8, start:stop]) for i in range(count)]
                for at, (i, j) in enumerate(pairs):
                    acc[at] = acc[at] + part[i] * part[j]
        return tuple(acc)

    def plane(z, acc):
        res_load(z, 0, y_local, z).wait()
        return add_rows(z, 0, y_local, acc)

    nothing = tuple(jnp.zeros((8, 128), jnp.float32) for _ in pairs)
    open_loads[0].wait()
    acc = add_rows(0, 0, half, nothing)
    open_loads[1].wait()
    acc = add_rows(0, half, y_local, acc)
    acc = lax.fori_loop(1, end_plane, plane, acc)
    for copy in loads[:3]:
        copy.wait()
    slot_count, entries = occ_ref.shape[1:]
    species = species_ref[...]
    orbitals = jnp.zeros_like(species)
    for species_index, orbital_number in enumerate(species_orbitals):
        orbitals = jnp.where(species == species_index, orbital_number, orbitals)
    square = (slot_count, slot_count)
    row_index = lax.broadcasted_iota(jnp.int32, square, 0)
    column_index = lax.broadcasted_iota(jnp.int32, square, 1)
    chosen = (row_index == column_index) & (column_index < live_ref[0])
    limit = jnp.sum(
        jnp.where(chosen, orbitals.astype(jnp.float32), 0.0), axis=1, keepdims=True
    )
    mask = (corner_ref[...] < limit).astype(jnp.float32)
    ratio = cells / (100.0 * slots)
    blocks_acc = [jnp.zeros((8, 128), jnp.float32) for _ in pairs]
    for first in range(0, slot_count, 8):
        for start, stop in lanes_of(entries):
            part = [
                wide(occ_res_ref[i, first:first + 8, start:stop] * mask[first:first + 8, start:stop])
                for i in range(count)
            ]
            for at, (i, j) in enumerate(pairs):
                blocks_acc[at] = blocks_acc[at] + part[i] * part[j]
    acc = [value + blocks * ratio for value, blocks in zip(acc, blocks_acc)]
    end_loads[0].wait()
    acc = add_rows(end_plane, 0, half, acc)
    end_loads[1].wait()
    acc = add_rows(end_plane, half, y_local, acc)

    for copy in loads[4:]:
        copy.start()
    stacked = jnp.concatenate([jnp.sum(a, axis=0, keepdims=True) for a in acc], axis=0)
    totals = jnp.sum(stacked, axis=1, keepdims=True) / cells
    shape = (len(pairs), 128)
    pair_index = lax.broadcasted_iota(jnp.int32, shape, 0)
    across = lax.broadcasted_iota(jnp.int32, shape, 1)
    packed = jnp.sum(jnp.where(pair_index == across, totals, 0.0), axis=0, keepdims=True)
    sums[pl.ds(me, 1), :] = packed

    pl.semaphore_wait(barrier, devices - 1)

    for spot, _ in partners:
        pltpu.make_async_remote_copy(
            src_ref=sums.at[pl.ds(me, 1)], dst_ref=sums.at[pl.ds(me, 1)],
            send_sem=sum_sem.at[0], recv_sem=sum_sem.at[1],
            device_id=spot, device_id_type=MESH,
        ).start()
    all_sums = pltpu.make_async_remote_copy(
        src_ref=sums.at[pl.ds(0, devices - 1)], dst_ref=sums.at[pl.ds(0, devices - 1)],
        send_sem=sum_sem.at[0], recv_sem=sum_sem.at[1],
        device_id=partners[0][0], device_id_type=MESH,
    )

    loads[3].wait()
    opening = slice(0, 2 * ends[0] * devices)

    left = (xf_ref[0, opening, :], xf_ref[1, opening, :])
    for i in range(count):
        history = split(res[i].reshape(z_local * y_local, x_length))
        first_turn[i] = three(left, history, ((1,), (1,)))

    all_sums.wait_recv()
    gathered = jnp.sum(sums[...], axis=0, keepdims=True)
    lane_index = lax.broadcasted_iota(jnp.int32, (1, 128), 1)
    entry = {
        pair: jnp.sum(jnp.where(lane_index == at, gathered, 0.0), axis=1, keepdims=True)
        for at, pair in enumerate(pairs)
    }
    weights = solve_weights(entry, count)

    def share(chunk, index):
        first, end = chunks[chunk]
        size = 2 * (end - first)
        return pl.ds(2 * first * devices + index * size, size)

    def go_copy(chunk, spot, target):
        return pltpu.make_async_remote_copy(
            src_ref=send_box.at[:, share(chunk, target), :],
            dst_ref=land_box.at[:, share(chunk, me), :],
            send_sem=go_send.at[0], recv_sem=go_recv.at[chunk],
            device_id=spot, device_id_type=MESH,
        )

    def landing(chunk, rows):
        if chunk < len(chunks) - 1:
            return field.at[:, rows, :]
        return last.at[:, pl.ds(rows.start - 2 * chunks[chunk][0] * devices, rows.size), :]

    def back_copy(chunk, spot, target):
        return pltpu.make_async_remote_copy(
            src_ref=back_box.at[:, share(chunk, target), :],
            dst_ref=landing(chunk, share(chunk, me)),
            send_sem=back_send.at[0], recv_sem=back_recv.at[chunk],
            device_id=spot, device_id_type=MESH,
        )

    def start_all(copy, chunk):
        for spot, target in partners:
            copy(chunk, spot, target).start()

    def whole(source, target, rows, send, recv):
        return pltpu.make_async_remote_copy(
            src_ref=source.at[:, rows, :], dst_ref=target.at[:, rows, :],
            send_sem=send, recv_sem=recv, device_id=partners[0][0], device_id_type=MESH,
        )

    def land_all(source, target, send, recv, chunk):
        first, end = chunks[chunk]
        rows = pl.ds(2 * first * devices, 2 * (end - first) * (devices - 1))
        whole(source, target, rows, send.at[0], recv.at[chunk]).wait_recv()

    def drain_all(source, target, send, recv):
        rows = pl.ds(0, freqs * (devices - 1))
        whole(source, target, rows, send.at[0], recv.at[0]).wait_send()

    def mixed(parts):
        total = weights[0] * parts[0]
        for i in range(1, count):
            total = total + weights[i] * parts[i]
        return total

    turned = mixed([first_turn[i] for i in range(count)])
    for t in range(tiles_out):
        send_box[t, opening, :] = turned[:, t * 128:(t + 1) * 128]
    start_all(go_copy, 0)
    land_box[:, share(0, me), :] = send_box[:, share(0, me), :]

    mixture = [mixed([res[i, z] for i in range(count)]) for z in range(z_local)]
    mixture = split(jnp.concatenate(mixture, axis=0))
    for chunk, (first, end) in enumerate(chunks):
        if chunk == 0:
            continue
        rows = slice(2 * first * devices, 2 * end * devices)
        turned = three((xf_ref[0, rows, :], xf_ref[1, rows, :]), mixture, ((1,), (1,)))
        for t in range(tiles_out):
            send_box[t, rows, :] = turned[:, t * 128:(t + 1) * 128]
        start_all(go_copy, chunk)
        land_box[:, share(chunk, me), :] = send_box[:, share(chunk, me), :]

    for copy in loads[4:]:
        copy.wait()
    for z in range(z_local):
        out_ref[z * y_local:(z + 1) * y_local, :] = mixed([dens[i, z] for i in range(count)])
    occ_out_ref[...] = mask * mixed(
        [occ_ref[i] + block_mixing * occ_res_ref[i] for i in range(count)]
    )
    all_sums.wait_send()

    z_forward = (zf_ref[0], zf_ref[1])
    z_back = (zb_ref[0], zb_ref[1])
    y_cosine = (yt_ref[0, 0], yt_ref[1, 0])
    y_sine = (yt_ref[0, 1], yt_ref[1, 1])
    shape = (2 * z_length, y_length)
    z_index = lax.rem(lax.broadcasted_iota(jnp.int32, shape, 0), z_length)
    y_index = lax.broadcasted_iota(jnp.int32, shape, 1)
    z_size = jnp.minimum(z_index, z_length - z_index).astype(jnp.float32)
    y_size = jnp.minimum(y_index, y_length - y_index).astype(jnp.float32)
    flat = z_size * z_size + y_size * y_size

    def filtered(wave, freq_x):
        size = freq_x.astype(jnp.float32)
        square = flat + size * size
        return split(wave * (square / (square + kerker_wave * kerker_wave)))

    for chunk, (first, end) in enumerate(chunks):
        size = 2 * (end - first)
        base = 2 * first * devices
        land_all(send_box, land_box, go_send, go_recv, chunk)
        for p in range(pencils):
            for f in range(size):
                joined = jnp.concatenate(
                    [
                        land_box[t, pl.ds(base + p * size + f, slabs, stride=pencils * size), :]
                        for t in range(tiles_out)
                    ],
                    axis=1,
                )
                for z in range(z_local):
                    planes[
                        2 * first + f, z * slabs:(z + 1) * slabs, p * y_local:(p + 1) * y_local
                    ] = joined[:, z * y_local:(z + 1) * y_local]
        block = split(planes[2 * first:2 * end].reshape(size * z_length, y_length))
        along_cosine = three(block, y_cosine, ((1,), (0,)))
        along_sine = three(block, y_sine, ((1,), (0,)))
        extra = first == 0
        for k in range(first, end):
            top, low = 2 * (k - first) * z_length, (2 * (k - first) + 1) * z_length
            stop = low + z_length
            real = along_cosine[top:low] + along_sine[low:stop]
            imag = along_cosine[low:stop] - along_sine[top:low]
            wave = three(z_forward, split(jnp.concatenate((real, imag), axis=0)), ((1,), (0,)))
            freq_x = me * slots_k + k
            spectrum[k - first] = three(z_back, filtered(wave, freq_x), ((1,), (0,)))
            if k == 0:
                freq_x = jnp.where(me == 0, x_length // 2, freq_x)
                spectrum[end] = three(z_back, filtered(wave, freq_x), ((1,), (0,)))
        used = end - first + (1 if extra else 0)
        block = split(spectrum[0:used].reshape(used * 2 * z_length, y_length))
        along_cosine = three(block, y_cosine, ((1,), (0,)))
        along_sine = three(block, y_sine, ((1,), (0,)))
        for k in range(first, end):
            top, low = 2 * (k - first) * z_length, (2 * (k - first) + 1) * z_length
            stop = low + z_length
            real = along_cosine[top:low] - along_sine[low:stop]
            if k == 0:
                top, low = 2 * end * z_length, (2 * end + 1) * z_length
                stop = low + z_length
            imag = along_cosine[low:stop] + along_sine[top:low]
            for c, part in enumerate((real, imag)):
                for p in range(pencils):
                    joined = jnp.concatenate(
                        [
                            part[z * slabs:(z + 1) * slabs, p * y_local:(p + 1) * y_local]
                            for z in range(z_local)
                        ],
                        axis=1,
                    )
                    start = base + p * size + 2 * (k - first) + c
                    for t in range(tiles_out):
                        back_box[t, pl.ds(start, slabs, stride=pencils * size), :] = joined[
                            :, t * 128:(t + 1) * 128
                        ]
        start_all(back_copy, chunk)
        landing(chunk, share(chunk, me))[...] = back_box[:, share(chunk, me), :]

    drain_all(send_box, land_box, go_send, go_recv)
    for chunk, (first, end) in enumerate(chunks):
        rows = pl.ds(2 * first * devices, 2 * (end - first) * (devices - 1))
        pltpu.make_async_remote_copy(
            src_ref=back_box.at[:, rows, :], dst_ref=landing(chunk, rows),
            send_sem=back_send.at[0], recv_sem=back_recv.at[chunk],
            device_id=partners[0][0], device_id_type=MESH,
        ).wait_recv()
        if chunk == len(chunks) - 1:
            continue
        used = slice(2 * first * devices, 2 * end * devices)
        table = (xb_ref[0, used, :], xb_ref[1, used, :])
        for t in range(tiles_out):
            rows = slice(t * 128, (t + 1) * 128)
            out_ref[rows, :] = out_ref[rows, :] + three(
                split(field[t, used, :]), table, ((0,), (0,))
            )
    drain_all(back_box, back_box, back_send, back_recv)


def finish_kernel(last, dens_ref, occ_ref, xb_ref, out_hbm, occ_hbm, out_ref, sem):
    tiles, depth, _ = last.shape
    copies = [pltpu.make_async_copy(occ_ref, occ_hbm, sem.at[tiles])]
    copies[0].start()
    dot = functools.partial(
        lax.dot_general,
        dimension_numbers=(((0,), (0,)), ((), ())),
        preferred_element_type=jnp.float32,
    )
    for first in range(0, tiles, GROUP):
        end = min(first + GROUP, tiles)
        high, low = split(jnp.concatenate([last[t] for t in range(first, end)], axis=1))
        both = jnp.concatenate((high, low), axis=0)
        turned = dot(both, xb_ref[:2 * depth]) + dot(high, xb_ref[2 * depth:])
        rows = slice(first * 128, end * 128)
        out_ref[rows, :] = dens_ref[rows, :] + turned
        copies.append(pltpu.make_async_copy(out_ref.at[rows], out_hbm.at[rows], sem.at[first]))
        copies[-1].start()
    for copy in copies:
        copy.wait()


def fused_body(
    density_history, residual_history, occupancy_history, occupancy_residual, species, slot_count
):
    count, z_local, y_local, x_length = residual_history.shape
    slabs = lax.axis_size("slab")
    pencils = lax.axis_size("pencil")
    devices = slabs * pencils
    z_length, y_length = z_local * slabs, y_local * pencils
    freqs = x_length // devices
    entry = np.arange(ORBITALS * ORBITALS)
    corner = np.maximum(entry // ORBITALS, entry % ORBITALS)[None].astype(np.float32)
    x_forward, x_back, *others = tables(x_length, y_length, z_length, pencils, slabs)
    constants = [x_forward, *others, x_back]
    ends = cuts_of(freqs // 2)
    chunks = len(ends)
    late = 2 * ends[-2] * devices if chunks > 1 else 0
    constants[-1] = x_back[:, :late] if late else x_back[:, :16]
    constants = [jnp.asarray(t) for t in constants]
    vmem = pl.BlockSpec(memory_space=pltpu.VMEM)
    hbm = pl.BlockSpec(memory_space=pltpu.HBM)
    box = (z_local * y_local // 128, devices * freqs, 128)
    sems = pltpu.SemaphoreType.DMA
    flat = jax.ShapeDtypeStruct((z_local * y_local, x_length), jnp.float32)
    blocks = jax.ShapeDtypeStruct(occupancy_history.shape[1:], jnp.float32)
    smalls = [
        occupancy_history, occupancy_residual, species[None], jnp.asarray(corner)
    ]
    mixed, mixed_blocks, last = pl.pallas_call(
        functools.partial(
            mix_kernel, slabs, pencils,
            z_length * y_length * x_length, species.shape[0] * devices,
        ),
        out_shape=(flat, blocks, jax.ShapeDtypeStruct((box[0], box[1] - late, 128), jnp.float32)),
        in_specs=[pl.BlockSpec(memory_space=pltpu.SMEM)] + [hbm] * (6 + len(constants)),
        out_specs=(vmem, vmem, vmem),
        scratch_shapes=[
            pltpu.VMEM(residual_history.shape, jnp.float32),
            pltpu.VMEM(residual_history.shape, jnp.float32),
            *[pltpu.VMEM(t.shape, t.dtype) for t in smalls],
            pltpu.VMEM((count, 2 * ends[0] * devices, z_local * y_local), jnp.float32),
            pltpu.VMEM((devices, 128), jnp.float32),
            pltpu.VMEM(box, jnp.float32),
            pltpu.VMEM(box, jnp.float32),
            pltpu.VMEM((freqs, z_length, y_length), jnp.float32),
            pltpu.VMEM((freqs // 2 + 1, 2 * z_length, y_length), jnp.float32),
            pltpu.VMEM(box, jnp.float32),
            pltpu.VMEM((box[0], late or 16, 128), jnp.float32),
            *[pltpu.VMEM(t.shape, t.dtype) for t in constants],
            sems((z_local + 2,)),
            sems((5 + len(constants),)),
            sems((2,)),
            sems((1,)), sems((chunks,)),
            sems((1,)), sems((chunks,)),
        ],
        compiler_params=pltpu.CompilerParams(
            collective_id=0, has_side_effects=True, vmem_limit_bytes=VMEM_LIMIT
        ),
    )(slot_count, *[
        pltpu.with_memory_space_constraint(value, pltpu.HBM)
        for value in (residual_history, density_history, *smalls, *constants)
    ])
    tiles = box[0]
    new_density, new_blocks = pl.pallas_call(
        finish_kernel,
        out_shape=(flat, blocks),
        in_specs=[vmem] * 4,
        out_specs=(hbm, hbm),
        scratch_shapes=[pltpu.VMEM(flat.shape, flat.dtype), sems((tiles + 1,))],
        compiler_params=pltpu.CompilerParams(vmem_limit_bytes=8 * 1024 * 1024),
    )(last, mixed, mixed_blocks, jnp.asarray(np.concatenate((x_back[0, late:], *x_back[:, late:]))))
    return new_density.reshape(z_local, y_local, x_length), new_blocks


def solution(mesh):
    placed = (
        P(None, "slab", "pencil", None),
        P(None, "slab", "pencil", None),
        P(None, ("slab", "pencil"), None),
        P(None, ("slab", "pencil"), None),
        P(("slab", "pencil")),
        P(("slab", "pencil")),
    )
    devices = mesh.shape["slab"] * mesh.shape["pencil"]

    def chosen(*arrays):
        x_length = arrays[0].shape[3]
        _, z_local, y_local, _ = arrays[0].shape
        fits = (
            x_length % (2 * devices) == 0
            and mesh.shape["slab"] % 8 == 0
            and y_local % 16 == 0
            and z_local * y_local % 128 == 0
            and z_local > 1
        )
        return (fused_body if fits else body)(*arrays)

    return jax.shard_map(
        chosen,
        mesh=mesh,
        in_specs=placed,
        out_specs=(P("slab", "pencil", None), P(("slab", "pencil"), None)),
        check_vma=False,
    )
```
